32 devices in a mesh: fsdp: 8 (over z, x), dp: 4 (over y, core).
Axes of the slice: x: 2, y: 2, z: 4, core: 2. Of those that a mesh axis runs over, the one named last changes fastest.
Arguments:
- tokens: bfloat16 [128, 96, 768], P(('fsdp', 'dp')), may hold values from -6 to 6
- memory: bfloat16 [128, 196, 768], P(('fsdp', 'dp')), may hold values from -6 to 6
- suffix_len: int32 [128], P(('fsdp', 'dp')), may hold values from 1 to 64, as said below
- cotangent: bfloat16 [128, 96, 768], P(('fsdp', 'dp')), may hold values from -6 to 6
- attn_in: bfloat16 [768, 2304], P(('fsdp', 'dp')), may hold values from -0.21875 to 0.21875
- attn_out: bfloat16 [768, 768], P(('fsdp', 'dp')), may hold values from -0.625 to 0.625
- cross_query: bfloat16 [768, 768], P(('fsdp', 'dp')), may hold values from -0.21875 to 0.21875
- cross_kv: bfloat16 [768, 1536], P(('fsdp', 'dp')), may hold values from -0.21875 to 0.21875
- cross_out: bfloat16 [768, 768], P(('fsdp', 'dp')), may hold values from -0.875 to 0.875
- mlp_in: bfloat16 [768, 3072], P(('fsdp', 'dp')), may hold values from -0.21875 to 0.21875
- mlp_out: bfloat16 [3072, 768], P(('fsdp', 'dp')), may hold values from -0.109375 to 0.109375
- ln_gain: bfloat16 [768, 3], P(('fsdp', 'dp')), may hold values from 0.25 to 1.75
- shifts: bfloat16 [768, 4], P(('fsdp', 'dp')), may hold values from -1.75 to 1.75
- mlp_bias: bfloat16 [3072], P(('fsdp', 'dp')), may hold values from -1.75 to 1.75
Outputs:
- layer_out: bfloat16 [128, 96, 768], P(('fsdp', 'dp'))
- input_grad: float32 [128, 96, 768], P(('fsdp', 'dp'))
- memory_grad: float32 [128, 196, 768], P(('fsdp', 'dp'))
- attn_in_grad: float32 [768, 2304], P(('fsdp', 'dp'))
- attn_out_grad: float32 [768, 768], P(('fsdp', 'dp'))
- cross_query_grad: float32 [768, 768], P(('fsdp', 'dp'))
- cross_kv_grad: float32 [768, 1536], P(('fsdp', 'dp'))
- cross_out_grad: float32 [768, 768], P(('fsdp', 'dp'))
- mlp_in_grad: float32 [768, 3072], P(('fsdp', 'dp'))
- mlp_out_grad: float32 [3072, 768], P(('fsdp', 'dp'))
- ln_gain_grad: float32 [768, 3], P(('fsdp', 'dp'))
- shifts_grad: float32 [768, 4], P(('fsdp', 'dp'))
- mlp_bias_grad: float32 [3072], P(('fsdp', 'dp'))
The draws below stay inside these ranges and needn't reach their ends.
Inputs may be any that keep to these rules, and one draw needn't show every extreme that they name: `suffix_len`: the number of live suffix tokens of each sequence, mostly under 10; some sequence has 64.
All inputs are finite; a program needn't handle non-finite values.
Results may differ from the reference program's by a relative error of at most 0.017.
Values may be sent and summed in bfloat16 or wider, within the bound.
No kernel may reach another device: no remote copies, remote signals or barrier semaphores. Data moves between devices by JAX's collectives and lax.ppermute only.
A program may use at most 192 MiB of HBM per device.

```python
import math
import jax
import jax.numpy as jnp
from jax import lax

D = 768
HEADS = 12
HEAD_DIM = 64
FF = 3072
MEM = 196
PREFIX = 32
SUFFIX_MAX = 64
LEN = 96
SEQS = 128


def draw_suffix_len(key, part):
    keys = jax.random.split(jax.random.fold_in(key, 17), 4)
    short = jax.random.randint(keys[0], (SEQS,), 1, min(10, SUFFIX_MAX + 1))
    tail = jax.random.randint(keys[1], (SEQS,), 1, SUFFIX_MAX + 1)
    pick = jax.random.randint(keys[2], (SEQS,), 0, 8) == 0
    lengths = jnp.where(pick, tail, short)
    spot = jax.random.randint(keys[3], (), 0, SEQS)
    lengths = jnp.where(jnp.arange(SEQS) == spot, SUFFIX_MAX, lengths)
    return lengths.astype(jnp.int32)


def shard_levels(key, extent, pieces, smallest, high):
    loudness, own = 1.0, jax.random.fold_in(key, 6)
    for dim, shards_of in pieces:
        draws = jnp.exp(jax.random.uniform(jax.random.fold_in(own, dim), (shards_of,), jnp.float32, smallest / len(pieces), high / len(pieces)))
        loudness = loudness * jnp.repeat(draws, extent[dim] // shards_of).reshape([-1 if axis == dim else 1 for axis in range(len(extent))])
    return loudness


def gaussian(key, extent, scale, bound, cuts=(), held_as=jnp.bfloat16):
    level = shard_levels(key, extent, cuts, -0.22, 0.18) if cuts else 1.0
    drawn = jax.random.normal(key, extent, jnp.float32) * scale * level
    return jnp.minimum(jnp.maximum(drawn, -bound), bound).astype(held_as)


def setup_inputs(seed: int = 0) -> dict:
    key_list = jax.random.split(jax.random.key(seed), 15)
    return {
        "tokens": gaussian(key_list[0], (SEQS, LEN, D), 1.0, 6.0, ((0, 32),)),
        "memory": gaussian(key_list[1], (SEQS, MEM, D), 1.0, 6.0, ((0, 32),)),
        "suffix_len": draw_suffix_len(jax.random.fold_in(key_list[14], 71), 0),
        "cotangent": gaussian(key_list[3], (SEQS, LEN, D), 1.0, 6.0, ((0, 32),)),
        "attn_in": gaussian(key_list[4], (D, 3 * D), D ** -0.5, 0.21875, ((0, 32),)),
        "attn_out": gaussian(key_list[5], (D, D), (D // 8) ** -0.5, 0.625, ((0, 32),)),
        "cross_query": gaussian(key_list[6], (D, D), D ** -0.5, 0.21875, ((0, 32),)),
        "cross_kv": gaussian(key_list[7], (D, 2 * D), D ** -0.5, 0.21875, ((0, 32),)),
        "cross_out": gaussian(key_list[8], (D, D), (D // 16) ** -0.5, 0.875, ((0, 32),)),
        "mlp_in": gaussian(key_list[9], (D, FF), D ** -0.5, 0.21875, ((0, 32),)),
        "mlp_out": gaussian(key_list[10], (FF, D), FF ** -0.5, 0.109375, ((0, 32),)),
        "ln_gain": jnp.clip(1.0 + 0.15 * jax.random.normal(key_list[11], (D, 3), jnp.float32), 0.25, 1.75).astype(jnp.bfloat16),
        "shifts": gaussian(key_list[12], (D, 4), 0.3, 1.75, ((0, 32),)),
        "mlp_bias": gaussian(key_list[13], (FF,), 0.3, 1.75, ((0, 32),)),
    }


EPS = 1e-05
TOP_PRECISION = lax.Precision.HIGHEST

@jax.custom_vjp
def low(v):
    return lax.optimization_barrier(v.astype(jnp.bfloat16)).astype(jnp.float32)

@jax.custom_vjp
def low_back(v):
    return v

def low_keep(v):
    return (low(v), None)

def low_pass(kept, grad):
    return (grad,)

def back_keep(v):
    return (v, None)

def back_low(kept, grad):
    return (low(grad),)
low.defvjp(low_keep, low_pass)
low_back.defvjp(back_keep, back_low)

def both_ways(value_tensor):
    return low_back(low(value_tensor))

def layer_norm(value_tensor, gain, shift):
    mean = lax.optimization_barrier(jnp.mean(value_tensor, axis=-1, keepdims=True))
    centred = value_tensor - mean
    spread = lax.optimization_barrier(jnp.mean(centred * centred, axis=-1, keepdims=True))
    return centred * lax.rsqrt(spread + EPS) * gain + shift

def project(value_tensor, weight_matrix):
    return jnp.einsum('owh,ht->owt', value_tensor, weight_matrix, precision=TOP_PRECISION)

def split_into_heads(value_tensor):
    seqs, rows, width = value_tensor.shape
    return value_tensor.reshape(seqs, rows, HEADS, HEAD_DIM)

def attend(query, key, value, allowed):
    raw = low_back(jnp.einsum('sqhe,skhe->shqk', query, key, precision=TOP_PRECISION))
    scores = raw * HEAD_DIM ** (-0.5)
    if allowed is not None:
        scores = jnp.where(allowed, scores, -1e+30)
    probs = low(jax.nn.softmax(scores, axis=-1))
    context = jnp.einsum('shqk,skhe->sqhe', probs, value, precision=TOP_PRECISION)
    seqs, rows = (context.shape[0], context.shape[1])
    return both_ways(context.reshape(seqs, rows, D))

def block_forward(params, stream0, memory, live):
    attn_in, attn_out, cross_query, cross_kv, cross_out, mlp_in, mlp_out, ln_gain, shifts, mlp_bias = params
    position = jnp.arange(LEN)
    causal = position[None, :] <= position[:, None]
    allowed = causal[None, None, :, :] & live[:, None, None, :]
    normed1 = low(layer_norm(stream0, ln_gain[:, 0], shifts[:, 0]))
    qkv = project(normed1, attn_in)
    query = split_into_heads(both_ways(qkv[..., :D]))
    key = split_into_heads(both_ways(qkv[..., D:2 * D]))
    value = split_into_heads(both_ways(qkv[..., 2 * D:]))
    context = attend(query, key, value, allowed)
    stream1 = stream0 + low_back(project(context, attn_out))
    normed2 = low(layer_norm(stream1, ln_gain[:, 1], shifts[:, 1]))
    cquery = split_into_heads(both_ways(project(normed2, cross_query)))
    ckv = project(memory, cross_kv)
    ckey = split_into_heads(both_ways(ckv[..., :D]))
    cvalue = split_into_heads(both_ways(ckv[..., D:]))
    ccontext = attend(cquery, ckey, cvalue, None)
    stream2 = stream1 + low_back(project(ccontext, cross_out))
    third_normalized = low(layer_norm(stream2, ln_gain[:, 2], shifts[:, 2]))
    pre = low_back(project(third_normalized, mlp_in) + mlp_bias)
    hidden = low(jax.nn.gelu(pre, approximate=True))
    return stream2 + low_back(project(hidden, mlp_out) + shifts[:, 3])

def reference(tokens, memory, suffix_len, cotangent, attn_in, attn_out, cross_query, cross_kv, cross_out, mlp_in, mlp_out, ln_gain, shifts, mlp_bias):
    params = tuple((w.astype(jnp.float32) for w in (attn_in, attn_out, cross_query, cross_kv, cross_out, mlp_in, mlp_out, ln_gain, shifts, mlp_bias)))
    position = jnp.arange(LEN).astype(jnp.int32)
    live = position[None, :] < (PREFIX + suffix_len.astype(jnp.int32))[:, None]
    group = math.gcd(SEQS, 32)
    count = SEQS // group

    def grouped(value_tensor):
        return value_tensor.reshape((count, group) + value_tensor.shape[1:])
    stream_groups = grouped(tokens.astype(jnp.float32))
    memory_groups = grouped(memory.astype(jnp.float32))
    live_groups = grouped(live)
    block_step = jax.checkpoint(block_forward)

    def whole(params, streams, memories):

        def scan_step(carry, inputs):
            stream, rows_mem, rows_live = inputs
            return (carry, block_step(params, stream, rows_mem, rows_live))
        _, outputs = lax.scan(scan_step, jnp.zeros((), jnp.float32), (streams, memories, live_groups))
        return outputs
    outputs, pull = jax.vjp(whole, params, stream_groups, memory_groups)
    start_grad = grouped(cotangent.astype(jnp.float32) * live[..., None].astype(jnp.float32))
    param_grads, stream_grad, memory_grad = pull(start_grad)
    layer_out = outputs.reshape(SEQS, LEN, D).astype(jnp.bfloat16)
    return (layer_out, stream_grad.reshape(SEQS, LEN, D), memory_grad.reshape(SEQS, MEM, D), param_grads[0], param_grads[1], param_grads[2], param_grads[3], param_grads[4], param_grads[5], param_grads[6], param_grads[7], param_grads[8], param_grads[9])
```

```python
import functools

import jax
import jax.numpy as jnp
from jax import lax
from jax.experimental import pallas as pl
from jax.experimental.pallas import tpu as pltpu
from jax.sharding import PartitionSpec as P

D = 768
HEADS = 12
HEAD_DIM = 64
PREFIX = 32


EPS = 1e-05


def norm_forward(value_tensor, gain, shift):
    mean = jnp.mean(value_tensor, axis=-1, keepdims=True)
    centred = value_tensor - mean
    spread = jnp.mean(centred * centred, axis=-1, keepdims=True)
    scale_inv = lax.rsqrt(spread + EPS)
    standard = centred * scale_inv
    return (standard * gain + shift, standard, scale_inv)


def norm_backward(upstream_gradient, standard, scale_inv, gain):
    grad_gain = jnp.sum(upstream_gradient * standard, axis=(0, 1))
    grad_shift = jnp.sum(upstream_gradient, axis=(0, 1))
    inner = upstream_gradient * gain
    first = jnp.mean(inner, axis=-1, keepdims=True)
    second = jnp.mean(inner * standard, axis=-1, keepdims=True)
    return (scale_inv * (inner - first - standard * second), grad_gain, grad_shift)


def project(value_tensor, weight_matrix):
    return jnp.einsum(
        "owh,ht->owt", value_tensor, weight_matrix, preferred_element_type=jnp.float32
    )


def back_project(upstream_gradient, weight_matrix):
    return jnp.einsum(
        "rmj,aj->rma", upstream_gradient, weight_matrix, preferred_element_type=jnp.float32
    )


def contract(value_tensor, upstream_gradient):
    return jnp.einsum(
        "xhq,xhg->qg", value_tensor, upstream_gradient, preferred_element_type=jnp.float32
    )


def scores_of(query, key, allowed):
    raw = jnp.einsum("sqhe,skhe->shqk", query, key, preferred_element_type=jnp.float32)
    scaled = raw * query.shape[-1] ** (-0.5)
    if allowed is None:
        return scaled
    return jnp.where(allowed, scaled, -1e30)


def attend_forward(query, key, value, allowed):
    scores = scores_of(query, key, allowed)
    top = jnp.max(scores, axis=-1, keepdims=True)
    weights = jnp.exp(scores - top)
    total = jnp.sum(weights, axis=-1, keepdims=True)
    probs = (weights / total).astype(jnp.bfloat16)
    context = jnp.einsum("shqk,skhe->sqhe", probs, value, preferred_element_type=jnp.float32)
    return (context.astype(jnp.bfloat16), top + jnp.log(total))


def attend_backward(query, key, value, allowed, summary, grad_context):
    probs = jnp.exp(scores_of(query, key, allowed) - summary)
    grad_probs = jnp.einsum(
        "sqhe,skhe->shqk", grad_context, value, preferred_element_type=jnp.float32
    )
    delta = jnp.sum(grad_probs * probs, axis=-1, keepdims=True)
    grad_scores = (probs * (grad_probs - delta) * query.shape[-1] ** (-0.5)).astype(jnp.bfloat16)
    grad_query = jnp.einsum("shqk,skhe->sqhe", grad_scores, key, preferred_element_type=jnp.float32)
    grad_key = jnp.einsum("shqk,sqhe->skhe", grad_scores, query, preferred_element_type=jnp.float32)
    grad_value = jnp.einsum(
        "shqk,sqhe->skhe",
        probs.astype(jnp.bfloat16),
        grad_context,
        preferred_element_type=jnp.float32,
    )
    return (grad_query, grad_key, grad_value)


AXES = ("fsdp", "dp")


def grid_rank(z, x, y, core):
    return ((z * 2 + x) * 2 + y) * 2 + core


def grid_perm(move):
    return [
        (grid_rank(z, x, y, core), grid_rank(*move(z, x, y, core)))
        for z in range(4)
        for x in range(2)
        for y in range(2)
        for core in range(2)
    ]


CORE = grid_perm(lambda z, x, y, core: (z, x, y, core ^ 1))
ZSHIFT = [
    grid_perm(lambda z, x, y, core, k=k: ((z + k) % 4, x, y, core)) for k in range(4)
]
FIRST = grid_perm(lambda z, x, y, core: (z, x ^ (1 - core), y ^ core, core))
SECOND = grid_perm(lambda z, x, y, core: (z, x ^ core, y ^ (1 - core), core))


def move(value, perm):
    return lax.ppermute(value, AXES, perm)


def place():
    outer, inner = lax.axis_index("fsdp"), lax.axis_index("dp")
    return outer // 2, outer % 2, inner // 2, inner % 2


def half_of(value, side):
    width = value.shape[1] // 2
    return lax.dynamic_slice_in_dim(value, side * width, width, axis=1)


def assemble_body(rows, widths, *refs):
    parts, outs, sem = refs[:8], refs[8:-1], refs[-1]
    z, x, y, core = place()
    copies = []
    for theirs in range(2):
        side = 1 - core if theirs else core
        for j in range(4):
            flip_x = (0, 1 - side, side, 1)[j]
            flip_y = (0, side, 1 - side, 1)[j]
            at_x = lax.rem(x + flip_x, 2)
            at_y = lax.rem(y + flip_y, 2)
            for k in range(4):
                at_z = lax.rem(z + 4 - k, 4)
                offset = 0
                for width, out in zip(widths, outs):
                    part = width // 2
                    target = pl.ds(pl.multiple_of(side * part, 128), part)
                    copies.append(
                        pltpu.make_async_copy(
                            parts[theirs * 4 + j].at[k, :, pl.ds(offset, part)],
                            out.at[at_z, at_x, at_y, :, target],
                            sem,
                        )
                    )
                    offset += part
    for copy in copies:
        copy.start()
    for copy in copies:
        copy.wait()


def assemble(parts, rows, widths):
    outs = pl.pallas_call(
        functools.partial(assemble_body, rows, widths),
        out_shape=[jax.ShapeDtypeStruct((4, 2, 2, 2 * rows, w), jnp.bfloat16) for w in widths],
        in_specs=[pl.BlockSpec(memory_space=pl.ANY)] * 8,
        out_specs=[pl.BlockSpec(memory_space=pl.ANY)] * len(widths),
        scratch_shapes=[pltpu.SemaphoreType.DMA],
        name="assemble",
    )(*parts)
    return [o.reshape(32 * rows, w) for o, w in zip(outs, widths)]


def gather_grid(shards):
    rows = shards[0].shape[0]
    core = place()[3]
    widths = [s.shape[1] for s in shards]
    left = jnp.concatenate([s[:, : w // 2] for s, w in zip(shards, widths)], axis=1)
    right = jnp.concatenate([s[:, w // 2 :] for s, w in zip(shards, widths)], axis=1)
    mine = jnp.where(core == 0, left, right)
    got = move(jnp.where(core == 0, right, left), CORE)
    pair = jnp.where(core == 0, jnp.concatenate([mine, got]), jnp.concatenate([got, mine]))
    line = jnp.stack([pair] + [move(pair, ZSHIFT[k]) for k in (1, 2, 3)])
    one = move(line, FIRST)
    two = move(line, SECOND)
    both = move(one, SECOND)
    parts = [line, one, two, both]
    parts = parts + [move(p, CORE) for p in parts]
    return assemble(parts, rows, widths)


def split_body(count, which, *refs):
    del which
    keeps, sends, outs = refs[: 2 * count], refs[2 * count : 4 * count], refs[4 * count :]
    for source, out in ((keeps, outs[0]), (sends, outs[1])):
        offset = 0
        for i in range(count):
            width = source[2 * i].shape[-1]
            total = source[2 * i][...].astype(jnp.float32) + source[2 * i + 1][...].astype(
                jnp.float32
            )
            out[:, :, :, offset : offset + width] = total.astype(jnp.bfloat16)
            offset += width


def split_add(pairs, rows):
    z, x, y, core = place()
    first = jnp.where(core == 0, x, y)
    second = jnp.where(core == 0, y, x)
    first_weight = jnp.where(core == 0, 2, 1)
    second_weight = 3 - first_weight
    which = jnp.stack(
        [
            (first ^ f) * first_weight + (second ^ s) * second_weight
            for s in range(2)
            for f in range(2)
        ]
    ).astype(jnp.int32)
    views, keep_specs, send_specs = [], [], []
    for keep, got in pairs:
        width = keep.shape[1]
        block = (4, 1, 2 * rows, width)
        for value in (keep, got):
            views.append(value.reshape(4, 4, 2 * rows, width))
            keep_specs.append(pl.BlockSpec(block, lambda f, which: (0, which[f], 0, 0)))
            send_specs.append(pl.BlockSpec(block, lambda f, which: (0, which[2 + f], 0, 0)))
    total = sum(keep.shape[1] for keep, _ in pairs)
    shape = jax.ShapeDtypeStruct((4, 2, 2 * rows, total), jnp.bfloat16)
    out_spec = pl.BlockSpec((4, 1, 2 * rows, total), lambda f, which: (0, f, 0, 0))
    return pl.pallas_call(
        functools.partial(split_body, len(pairs)),
        out_shape=[shape, shape],
        grid_spec=pltpu.PrefetchScalarGridSpec(
            num_scalar_prefetch=1,
            grid=(2,),
            in_specs=keep_specs + send_specs,
            out_specs=[out_spec, out_spec],
        ),
        name="split_add",
    )(which, *views, *views)


def reduce_grid(factors):
    z, x, y, core = place()
    pairs = []
    rows = factors[0][0].shape[1] // 32
    for value, upstream in factors:
        send = contract_low(value, half_of(upstream, 1 - core))
        got = move(send, CORE)
        keep = contract_low(value, half_of(upstream, core))
        pairs.append((keep, got))
    keep, send = split_add(pairs, rows)
    got = move(send, SECOND)
    f32 = jnp.float32
    got_first = move(
        (keep[:, 1].astype(f32) + got[:, 1].astype(f32)).astype(jnp.bfloat16), FIRST
    )
    def plane(k):
        at = (z + k) % 4
        pick = lambda v: lax.dynamic_index_in_dim(v, at, 0, keepdims=False).astype(f32)
        return pick(keep[:, 0]) + pick(got[:, 0]) + pick(got_first)

    total = plane(0)
    for k in (1, 2, 3):
        total = total + move(plane(k).astype(jnp.bfloat16), ZSHIFT[k]).astype(f32)
    mine = lax.dynamic_slice_in_dim(total, core * rows, rows, axis=0)
    other = move(lax.dynamic_slice_in_dim(total, (1 - core) * rows, rows, axis=0), CORE)
    left = jnp.where(core == 0, mine, other)
    right = jnp.where(core == 0, other, mine)
    results = []
    offset = 0
    for keep_part, _ in pairs:
        width = keep_part.shape[1]
        results.append(
            jnp.concatenate(
                [left[:, offset : offset + width], right[:, offset : offset + width]], axis=1
            )
        )
        offset += width
    return results


def contract_low(value, upstream_gradient):
    return lax.dot_general(
        value,
        upstream_gradient,
        (((0,), (0,)), ((), ())),
        preferred_element_type=jnp.float32,
    ).astype(jnp.bfloat16)


def gather_plain(shards):
    widths = [s.shape[1] for s in shards]
    whole = lax.all_gather(jnp.concatenate(shards, axis=1), AXES, axis=0, tiled=True)
    results = []
    offset = 0
    for width in widths:
        results.append(whole[:, offset : offset + width])
        offset += width
    return results


def reduce_plain(factors):
    packed = jnp.concatenate([contract_low(v, u) for v, u in factors], axis=1)
    summed = lax.psum_scatter(packed, AXES, scatter_dimension=0, tiled=True).astype(jnp.float32)
    results = []
    offset = 0
    for _, u in factors:
        results.append(summed[:, offset : offset + u.shape[1]])
        offset += u.shape[1]
    return results


def local(
    gather,
    reduce,
    tokens,
    memory,
    suffix_len,
    cotangent,
    attn_in,
    attn_out,
    cross_query,
    cross_kv,
    cross_out,
    mlp_in,
    mlp_out,
    ln_gain,
    shifts,
    mlp_bias,
):
    owned = attn_in.shape[0]
    small = jnp.concatenate(
        [
            ln_gain,
            shifts,
            mlp_bias.reshape(owned, 4),
            jnp.zeros((owned, 256 - 11), jnp.bfloat16),
        ],
        axis=1,
    )
    w_qkv, smalls = gather([attn_in, small])
    w_out, w_cquery, w_ckv, w_cout = gather([attn_out, cross_query, cross_kv, cross_out])
    (w_in,) = gather([mlp_in])
    (w_down,) = gather([mlp_out])
    gains, biases, hidden_bias = smalls[:, :3], smalls[:, 3:7], smalls[:, 7:11].reshape(-1)
    seqs, rows, width = tokens.shape
    position = jnp.arange(rows)
    live = position[None, :] < (PREFIX + suffix_len)[:, None]
    allowed = (position[None, :] <= position[:, None])[None, None, :, :] & live[:, None, None, :]
    gain_vals = gains.astype(jnp.float32)
    bias_vals = biases.astype(jnp.float32)
    stream0 = tokens.astype(jnp.float32)
    normed1, standard1, inverse1 = norm_forward(stream0, gain_vals[:, 0], bias_vals[:, 0])
    normed1 = normed1.astype(jnp.bfloat16)
    qkv = project(normed1, w_qkv).astype(jnp.bfloat16)
    query = qkv[..., :D].reshape(seqs, rows, HEADS, HEAD_DIM)
    key = qkv[..., D : 2 * D].reshape(seqs, rows, HEADS, HEAD_DIM)
    value = qkv[..., 2 * D :].reshape(seqs, rows, HEADS, HEAD_DIM)
    context, first_statistics = attend_forward(query, key, value, allowed)
    joined = context.reshape(seqs, rows, D)
    stream1 = stream0 + project(joined, w_out)
    normed2, standard2, inverse2 = norm_forward(stream1, gain_vals[:, 1], bias_vals[:, 1])
    normed2 = normed2.astype(jnp.bfloat16)
    cquery = project(normed2, w_cquery).astype(jnp.bfloat16).reshape(seqs, rows, HEADS, HEAD_DIM)
    ckv = project(memory, w_ckv).astype(jnp.bfloat16)
    mem_rows = memory.shape[1]
    ckey = ckv[..., :D].reshape(seqs, mem_rows, HEADS, HEAD_DIM)
    cvalue = ckv[..., D:].reshape(seqs, mem_rows, HEADS, HEAD_DIM)
    ccontext, summary2 = attend_forward(cquery, ckey, cvalue, None)
    cjoined = ccontext.reshape(seqs, rows, D)
    stream2 = stream1 + project(cjoined, w_cout)
    third_normalized, standard3, inverse3 = norm_forward(stream2, gain_vals[:, 2], bias_vals[:, 2])
    third_normalized = third_normalized.astype(jnp.bfloat16)
    pre = project(third_normalized, w_in) + hidden_bias.astype(jnp.float32)
    activated = jax.nn.gelu(pre, approximate=True).astype(jnp.bfloat16)
    layer_out = (stream2 + project(activated, w_down) + bias_vals[:, 3]).astype(jnp.bfloat16)
    upstream_gradient = cotangent.astype(jnp.float32) * live[..., None].astype(jnp.float32)
    grad_low = upstream_gradient.astype(jnp.bfloat16)
    flat = lambda v: v.reshape(-1, v.shape[-1])
    (mlp_out_grad,) = reduce([(flat(activated), flat(grad_low))])
    g_out_bias = jnp.sum(grad_low, axis=(0, 1), dtype=jnp.float32)
    grad_act = back_project(grad_low, w_down)
    _, gelu_back = jax.vjp(lambda v: jax.nn.gelu(v, approximate=True), pre)
    grad_pre = gelu_back(grad_act)[0].astype(jnp.bfloat16)
    g_hidden_bias = jnp.sum(grad_pre, axis=(0, 1), dtype=jnp.float32)
    (mlp_in_grad,) = reduce([(flat(third_normalized), flat(grad_pre))])
    grad_back, g_gain3, g_shift3 = norm_backward(
        back_project(grad_pre, w_in), standard3, inverse3, gain_vals[:, 2]
    )
    upstream_gradient = upstream_gradient + grad_back
    grad_low = upstream_gradient.astype(jnp.bfloat16)
    cout_factors = (flat(cjoined), flat(grad_low))
    grad_cctx = (
        back_project(grad_low, w_cout).astype(jnp.bfloat16).reshape(seqs, rows, HEADS, HEAD_DIM)
    )
    grad_cq, grad_ck, grad_cv = attend_backward(cquery, ckey, cvalue, None, summary2, grad_cctx)
    grad_cq = grad_cq.astype(jnp.bfloat16).reshape(seqs, rows, D)
    grad_ckv = jnp.concatenate(
        (grad_ck.reshape(seqs, mem_rows, D), grad_cv.reshape(seqs, mem_rows, D)), axis=-1
    ).astype(jnp.bfloat16)
    cross_query_grad, cross_kv_grad, cross_out_grad = reduce(
        [(flat(normed2), flat(grad_cq)), (flat(memory), flat(grad_ckv)), cout_factors]
    )
    memory_grad = back_project(grad_ckv, w_ckv)
    grad_back, g_gain2, g_shift2 = norm_backward(
        back_project(grad_cq, w_cquery), standard2, inverse2, gain_vals[:, 1]
    )
    upstream_gradient = upstream_gradient + grad_back
    grad_low = upstream_gradient.astype(jnp.bfloat16)
    out_factors = (flat(joined), flat(grad_low))
    grad_ctx = (
        back_project(grad_low, w_out).astype(jnp.bfloat16).reshape(seqs, rows, HEADS, HEAD_DIM)
    )
    grad_q, grad_k, grad_v = attend_backward(query, key, value, allowed, first_statistics, grad_ctx)
    grad_qkv = jnp.concatenate(
        (
            grad_q.reshape(seqs, rows, D),
            grad_k.reshape(seqs, rows, D),
            grad_v.reshape(seqs, rows, D),
        ),
        axis=-1,
    ).astype(jnp.bfloat16)
    grad_back, g_gain1, g_shift1 = norm_backward(
        back_project(grad_qkv, w_qkv), standard1, inverse1, gain_vals[:, 0]
    )
    input_grad = upstream_gradient + grad_back
    small_sums = jnp.stack(
        (g_gain1, g_gain2, g_gain3, g_shift1, g_shift2, g_shift3, g_out_bias), axis=0
    )
    bias_sums = g_hidden_bias.reshape(D, 4).T
    sums = jnp.concatenate([small_sums, bias_sums], axis=0)
    picks = jnp.eye(11, 256, dtype=jnp.bfloat16)
    attn_in_grad, attn_out_grad, small_grad = reduce(
        [(flat(normed1), flat(grad_qkv)), out_factors, (sums.astype(jnp.bfloat16), picks)]
    )
    return (
        layer_out,
        input_grad,
        memory_grad,
        attn_in_grad,
        attn_out_grad,
        cross_query_grad,
        cross_kv_grad,
        cross_out_grad,
        mlp_in_grad,
        mlp_out_grad,
        small_grad[:, :3],
        small_grad[:, 3:7],
        small_grad[:, 7:11].reshape(-1),
    )


def solution(mesh):
    in_specs = (
        P(("fsdp", "dp"), None, None),
        P(("fsdp", "dp"), None, None),
        P(("fsdp", "dp")),
        P(("fsdp", "dp"), None, None),
        P(("fsdp", "dp"), None),
        P(("fsdp", "dp"), None),
        P(("fsdp", "dp"), None),
        P(("fsdp", "dp"), None),
        P(("fsdp", "dp"), None),
        P(("fsdp", "dp"), None),
        P(("fsdp", "dp"), None),
        P(("fsdp", "dp"), None),
        P(("fsdp", "dp"), None),
        P(("fsdp", "dp")),
    )
    out_specs = (
        P(("fsdp", "dp"), None, None),
        P(("fsdp", "dp"), None, None),
        P(("fsdp", "dp"), None, None),
        P(("fsdp", "dp"), None),
        P(("fsdp", "dp"), None),
        P(("fsdp", "dp"), None),
        P(("fsdp", "dp"), None),
        P(("fsdp", "dp"), None),
        P(("fsdp", "dp"), None),
        P(("fsdp", "dp"), None),
        P(("fsdp", "dp"), None),
        P(("fsdp", "dp"), None),
        P(("fsdp", "dp")),
    )
    if dict(mesh.shape) == {"fsdp": 8, "dp": 4}:
        program = functools.partial(local, gather_grid, reduce_grid)
    else:
        program = functools.partial(local, gather_plain, reduce_plain)
    return jax.shard_map(program, mesh=mesh, in_specs=in_specs, out_specs=out_specs, check_vma=False)
```

```python
import functools

import jax
import jax.numpy as jnp
from jax import lax
from jax.experimental import pallas as pl
from jax.experimental.pallas import tpu as pltpu
from jax.sharding import PartitionSpec as P

D = 768
HEADS = 12
HEAD_DIM = 64
PREFIX = 32


EPS = 1e-05


def norm_forward(value_tensor, gain, shift):
    mean = jnp.mean(value_tensor, axis=-1, keepdims=True)
    centred = value_tensor - mean
    spread = jnp.mean(centred * centred, axis=-1, keepdims=True)
    scale_inv = lax.rsqrt(spread + EPS)
    standard = centred * scale_inv
    return (standard * gain + shift, standard, scale_inv)


def norm_backward(upstream_gradient, standard, scale_inv, gain):
    grad_gain = jnp.sum(upstream_gradient * standard, axis=(0, 1))
    grad_shift = jnp.sum(upstream_gradient, axis=(0, 1))
    inner = upstream_gradient * gain
    first = jnp.mean(inner, axis=-1, keepdims=True)
    second = jnp.mean(inner * standard, axis=-1, keepdims=True)
    return (scale_inv * (inner - first - standard * second), grad_gain, grad_shift)


def project(value_tensor, weight_matrix):
    return jnp.einsum(
        "owh,ht->owt", value_tensor, weight_matrix, preferred_element_type=jnp.float32
    )


def back_project(upstream_gradient, weight_matrix):
    return jnp.einsum(
        "rmj,aj->rma", upstream_gradient, weight_matrix, preferred_element_type=jnp.float32
    )


def contract(value_tensor, upstream_gradient):
    return jnp.einsum(
        "xhq,xhg->qg", value_tensor, upstream_gradient, preferred_element_type=jnp.float32
    )


def scores_of(query, key, allowed):
    raw = jnp.einsum("sqhe,skhe->shqk", query, key, preferred_element_type=jnp.float32)
    scaled = raw * query.shape[-1] ** (-0.5)
    if allowed is None:
        return scaled
    return jnp.where(allowed, scaled, -1e30)


def attend_forward(query, key, value, allowed):
    scores = scores_of(query, key, allowed)
    top = jnp.max(scores, axis=-1, keepdims=True)
    weights = jnp.exp(scores - top)
    total = jnp.sum(weights, axis=-1, keepdims=True)
    probs = (weights / total).astype(jnp.bfloat16)
    context = jnp.einsum("shqk,skhe->sqhe", probs, value, preferred_element_type=jnp.float32)
    return (context.astype(jnp.bfloat16), top + jnp.log(total))


def attend_backward(query, key, value, allowed, summary, grad_context):
    probs = jnp.exp(scores_of(query, key, allowed) - summary)
    grad_probs = jnp.einsum(
        "sqhe,skhe->shqk", grad_context, value, preferred_element_type=jnp.float32
    )
    delta = jnp.sum(grad_probs * probs, axis=-1, keepdims=True)
    grad_scores = (probs * (grad_probs - delta) * query.shape[-1] ** (-0.5)).astype(jnp.bfloat16)
    grad_query = jnp.einsum("shqk,skhe->sqhe", grad_scores, key, preferred_element_type=jnp.float32)
    grad_key = jnp.einsum("shqk,sqhe->skhe", grad_scores, query, preferred_element_type=jnp.float32)
    grad_value = jnp.einsum(
        "shqk,sqhe->skhe",
        probs.astype(jnp.bfloat16),
        grad_context,
        preferred_element_type=jnp.float32,
    )
    return (grad_query, grad_key, grad_value)


AXES = ("fsdp", "dp")


def grid_rank(z, x, y, core):
    return ((z * 2 + x) * 2 + y) * 2 + core


def grid_perm(move):
    return [
        (grid_rank(z, x, y, core), grid_rank(*move(z, x, y, core)))
        for z in range(4)
        for x in range(2)
        for y in range(2)
        for core in range(2)
    ]


CORE = grid_perm(lambda z, x, y, core: (z, x, y, core ^ 1))
ZSHIFT = [
    grid_perm(lambda z, x, y, core, k=k: ((z + k) % 4, x, y, core)) for k in range(4)
]
FIRST = grid_perm(lambda z, x, y, core: (z, x ^ (1 - core), y ^ core, core))
SECOND = grid_perm(lambda z, x, y, core: (z, x ^ core, y ^ (1 - core), core))


def move(value, perm):
    return lax.ppermute(value, AXES, perm)


def place():
    outer, inner = lax.axis_index("fsdp"), lax.axis_index("dp")
    return outer // 2, outer % 2, inner // 2, inner % 2


def half_of(value, side):
    width = value.shape[1] // 2
    return lax.dynamic_slice_in_dim(value, side * width, width, axis=1)


def assemble_body(widths, spot, *refs):
    parts, outs = refs[:8], refs[8:]
    x, y, core = spot[1], spot[2], spot[3]

    def place_all(mine):
        for theirs in range(2):
            side = 1 - mine if theirs else mine
            for j in range(4):
                flip_x = (0, 1 - side, side, 1)[j]
                flip_y = (0, side, 1 - side, 1)[j]
                offset = 0
                for width, out in zip(widths, outs):
                    part = width // 2
                    out[0, x ^ flip_x, y ^ flip_y, :, side * part : (side + 1) * part] = parts[
                        theirs * 4 + j
                    ][0, :, offset : offset + part]
                    offset += part

    @pl.when(core == 0)
    def _():
        place_all(0)

    @pl.when(core == 1)
    def _():
        place_all(1)


def assemble(parts, rows, widths, spot):
    half = sum(widths) // 2
    outs = pl.pallas_call(
        functools.partial(assemble_body, widths),
        out_shape=[jax.ShapeDtypeStruct((4, 2, 2, 2 * rows, w), jnp.bfloat16) for w in widths],
        grid_spec=pltpu.PrefetchScalarGridSpec(
            num_scalar_prefetch=1,
            grid=(4,),
            in_specs=[pl.BlockSpec((1, 2 * rows, half), lambda k, spot: (k, 0, 0))] * 8,
            out_specs=[
                pl.BlockSpec(
                    (1, 2, 2, 2 * rows, w),
                    lambda k, spot: (lax.rem(spot[0] + 4 - k, 4), 0, 0, 0, 0),
                )
                for w in widths
            ],
        ),
        name="assemble",
    )(spot, *parts)
    return [o.reshape(32 * rows, w) for o, w in zip(outs, widths)]


def gather_grid(shards):
    rows = shards[0].shape[0]
    core = place()[3]
    widths = [s.shape[1] for s in shards]
    left = jnp.concatenate([s[:, : w // 2] for s, w in zip(shards, widths)], axis=1)
    right = jnp.concatenate([s[:, w // 2 :] for s, w in zip(shards, widths)], axis=1)
    mine = jnp.where(core == 0, left, right)
    got = move(jnp.where(core == 0, right, left), CORE)
    pair = jnp.where(core == 0, jnp.concatenate([mine, got]), jnp.concatenate([got, mine]))
    line = jnp.stack([pair] + [move(pair, ZSHIFT[k]) for k in (1, 2, 3)])
    one = move(line, FIRST)
    two = move(line, SECOND)
    both = move(one, SECOND)
    parts = [line, one, two, both]
    parts = parts + [move(p, CORE) for p in parts]
    return assemble(parts, rows, widths, jnp.stack(place()).astype(jnp.int32))


def split_body(count, which, *refs):
    del which
    keeps, sends, outs = refs[: 2 * count], refs[2 * count : 4 * count], refs[4 * count :]
    for source, out in ((keeps, outs[0]), (sends, outs[1])):
        offset = 0
        for i in range(count):
            width = source[2 * i].shape[-1]
            total = source[2 * i][...].astype(jnp.float32) + source[2 * i + 1][...].astype(
                jnp.float32
            )
            out[:, :, :, offset : offset + width] = total.astype(jnp.bfloat16)
            offset += width


def split_add(pairs, rows):
    z, x, y, core = place()
    first = jnp.where(core == 0, x, y)
    second = jnp.where(core == 0, y, x)
    first_weight = jnp.where(core == 0, 2, 1)
    second_weight = 3 - first_weight
    which = jnp.stack(
        [
            (first ^ f) * first_weight + (second ^ s) * second_weight
            for s in range(2)
            for f in range(2)
        ]
    ).astype(jnp.int32)
    views, keep_specs, send_specs = [], [], []
    for keep, got in pairs:
        width = keep.shape[1]
        block = (4, 1, 2 * rows, width)
        for value in (keep, got):
            views.append(value.reshape(4, 4, 2 * rows, width))
            keep_specs.append(pl.BlockSpec(block, lambda f, which: (0, which[f], 0, 0)))
            send_specs.append(pl.BlockSpec(block, lambda f, which: (0, which[2 + f], 0, 0)))
    total = sum(keep.shape[1] for keep, _ in pairs)
    shape = jax.ShapeDtypeStruct((4, 2, 2 * rows, total), jnp.bfloat16)
    out_spec = pl.BlockSpec((4, 1, 2 * rows, total), lambda f, which: (0, f, 0, 0))
    return pl.pallas_call(
        functools.partial(split_body, len(pairs)),
        out_shape=[shape, shape],
        grid_spec=pltpu.PrefetchScalarGridSpec(
            num_scalar_prefetch=1,
            grid=(2,),
            in_specs=keep_specs + send_specs,
            out_specs=[out_spec, out_spec],
        ),
        name="split_add",
    )(which, *views, *views)


def reduce_grid(factors):
    z, x, y, core = place()
    pairs = []
    rows = factors[0][0].shape[1] // 32
    for value, upstream in factors:
        send = contract_low(value, half_of(upstream, 1 - core))
        got = move(send, CORE)
        keep = contract_low(value, half_of(upstream, core))
        pairs.append((keep, got))
    keep, send = split_add(pairs, rows)
    got = move(send, SECOND)
    f32 = jnp.float32
    got_first = move(
        (keep[:, 1].astype(f32) + got[:, 1].astype(f32)).astype(jnp.bfloat16), FIRST
    )
    def plane(k):
        at = (z + k) % 4
        pick = lambda v: lax.dynamic_index_in_dim(v, at, 0, keepdims=False).astype(f32)
        return pick(keep[:, 0]) + pick(got[:, 0]) + pick(got_first)

    total = plane(0)
    for k in (1, 2, 3):
        total = total + move(plane(k).astype(jnp.bfloat16), ZSHIFT[k]).astype(f32)
    mine = lax.dynamic_slice_in_dim(total, core * rows, rows, axis=0)
    other = move(lax.dynamic_slice_in_dim(total, (1 - core) * rows, rows, axis=0), CORE)
    left = jnp.where(core == 0, mine, other)
    right = jnp.where(core == 0, other, mine)
    results = []
    offset = 0
    for keep_part, _ in pairs:
        width = keep_part.shape[1]
        results.append(
            jnp.concatenate(
                [left[:, offset : offset + width], right[:, offset : offset + width]], axis=1
            )
        )
        offset += width
    return results


def contract_low(value, upstream_gradient):
    return lax.dot_general(
        value,
        upstream_gradient,
        (((0,), (0,)), ((), ())),
        preferred_element_type=jnp.float32,
    ).astype(jnp.bfloat16)


def gather_plain(shards):
    widths = [s.shape[1] for s in shards]
    whole = lax.all_gather(jnp.concatenate(shards, axis=1), AXES, axis=0, tiled=True)
    results = []
    offset = 0
    for width in widths:
        results.append(whole[:, offset : offset + width])
        offset += width
    return results


def reduce_plain(factors):
    packed = jnp.concatenate([contract_low(v, u) for v, u in factors], axis=1)
    summed = lax.psum_scatter(packed, AXES, scatter_dimension=0, tiled=True).astype(jnp.float32)
    results = []
    offset = 0
    for _, u in factors:
        results.append(summed[:, offset : offset + u.shape[1]])
        offset += u.shape[1]
    return results


def local(
    gather,
    reduce,
    tokens,
    memory,
    suffix_len,
    cotangent,
    attn_in,
    attn_out,
    cross_query,
    cross_kv,
    cross_out,
    mlp_in,
    mlp_out,
    ln_gain,
    shifts,
    mlp_bias,
):
    owned = attn_in.shape[0]
    small = jnp.concatenate(
        [
            ln_gain,
            shifts,
            mlp_bias.reshape(owned, 4),
            jnp.zeros((owned, 256 - 11), jnp.bfloat16),
        ],
        axis=1,
    )
    w_qkv, smalls = gather([attn_in, small])
    w_out, w_cquery, w_ckv, w_cout = gather([attn_out, cross_query, cross_kv, cross_out])
    (w_in,) = gather([mlp_in])
    (w_down,) = gather([mlp_out])
    gains, biases, hidden_bias = smalls[:, :3], smalls[:, 3:7], smalls[:, 7:11].reshape(-1)
    seqs, rows, width = tokens.shape
    position = jnp.arange(rows)
    live = position[None, :] < (PREFIX + suffix_len)[:, None]
    allowed = (position[None, :] <= position[:, None])[None, None, :, :] & live[:, None, None, :]
    gain_vals = gains.astype(jnp.float32)
    bias_vals = biases.astype(jnp.float32)
    stream0 = tokens.astype(jnp.float32)
    normed1, standard1, inverse1 = norm_forward(stream0, gain_vals[:, 0], bias_vals[:, 0])
    normed1 = normed1.astype(jnp.bfloat16)
    qkv = project(normed1, w_qkv).astype(jnp.bfloat16)
    query = qkv[..., :D].reshape(seqs, rows, HEADS, HEAD_DIM)
    key = qkv[..., D : 2 * D].reshape(seqs, rows, HEADS, HEAD_DIM)
    value = qkv[..., 2 * D :].reshape(seqs, rows, HEADS, HEAD_DIM)
    context, first_statistics = attend_forward(query, key, value, allowed)
    joined = context.reshape(seqs, rows, D)
    stream1 = stream0 + project(joined, w_out)
    normed2, standard2, inverse2 = norm_forward(stream1, gain_vals[:, 1], bias_vals[:, 1])
    normed2 = normed2.astype(jnp.bfloat16)
    cquery = project(normed2, w_cquery).astype(jnp.bfloat16).reshape(seqs, rows, HEADS, HEAD_DIM)
    ckv = project(memory, w_ckv).astype(jnp.bfloat16)
    mem_rows = memory.shape[1]
    ckey = ckv[..., :D].reshape(seqs, mem_rows, HEADS, HEAD_DIM)
    cvalue = ckv[..., D:].reshape(seqs, mem_rows, HEADS, HEAD_DIM)
    ccontext, summary2 = attend_forward(cquery, ckey, cvalue, None)
    cjoined = ccontext.reshape(seqs, rows, D)
    stream2 = stream1 + project(cjoined, w_cout)
    third_normalized, standard3, inverse3 = norm_forward(stream2, gain_vals[:, 2], bias_vals[:, 2])
    third_normalized = third_normalized.astype(jnp.bfloat16)
    pre = project(third_normalized, w_in) + hidden_bias.astype(jnp.float32)
    activated = jax.nn.gelu(pre, approximate=True).astype(jnp.bfloat16)
    layer_out = (stream2 + project(activated, w_down) + bias_vals[:, 3]).astype(jnp.bfloat16)
    upstream_gradient = cotangent.astype(jnp.float32) * live[..., None].astype(jnp.float32)
    grad_low = upstream_gradient.astype(jnp.bfloat16)
    flat = lambda v: v.reshape(-1, v.shape[-1])
    (mlp_out_grad,) = reduce([(flat(activated), flat(grad_low))])
    g_out_bias = jnp.sum(grad_low, axis=(0, 1), dtype=jnp.float32)
    grad_act = back_project(grad_low, w_down)
    _, gelu_back = jax.vjp(lambda v: jax.nn.gelu(v, approximate=True), pre)
    grad_pre = gelu_back(grad_act)[0].astype(jnp.bfloat16)
    g_hidden_bias = jnp.sum(grad_pre, axis=(0, 1), dtype=jnp.float32)
    (mlp_in_grad,) = reduce([(flat(third_normalized), flat(grad_pre))])
    grad_back, g_gain3, g_shift3 = norm_backward(
        back_project(grad_pre, w_in), standard3, inverse3, gain_vals[:, 2]
    )
    upstream_gradient = upstream_gradient + grad_back
    grad_low = upstream_gradient.astype(jnp.bfloat16)
    cout_factors = (flat(cjoined), flat(grad_low))
    grad_cctx = (
        back_project(grad_low, w_cout).astype(jnp.bfloat16).reshape(seqs, rows, HEADS, HEAD_DIM)
    )
    grad_cq, grad_ck, grad_cv = attend_backward(cquery, ckey, cvalue, None, summary2, grad_cctx)
    grad_cq = grad_cq.astype(jnp.bfloat16).reshape(seqs, rows, D)
    grad_ckv = jnp.concatenate(
        (grad_ck.reshape(seqs, mem_rows, D), grad_cv.reshape(seqs, mem_rows, D)), axis=-1
    ).astype(jnp.bfloat16)
    cross_query_grad, cross_kv_grad, cross_out_grad = reduce(
        [(flat(normed2), flat(grad_cq)), (flat(memory), flat(grad_ckv)), cout_factors]
    )
    memory_grad = back_project(grad_ckv, w_ckv)
    grad_back, g_gain2, g_shift2 = norm_backward(
        back_project(grad_cq, w_cquery), standard2, inverse2, gain_vals[:, 1]
    )
    upstream_gradient = upstream_gradient + grad_back
    grad_low = upstream_gradient.astype(jnp.bfloat16)
    out_factors = (flat(joined), flat(grad_low))
    grad_ctx = (
        back_project(grad_low, w_out).astype(jnp.bfloat16).reshape(seqs, rows, HEADS, HEAD_DIM)
    )
    grad_q, grad_k, grad_v = attend_backward(query, key, value, allowed, first_statistics, grad_ctx)
    grad_qkv = jnp.concatenate(
        (
            grad_q.reshape(seqs, rows, D),
            grad_k.reshape(seqs, rows, D),
            grad_v.reshape(seqs, rows, D),
        ),
        axis=-1,
    ).astype(jnp.bfloat16)
    grad_back, g_gain1, g_shift1 = norm_backward(
        back_project(grad_qkv, w_qkv), standard1, inverse1, gain_vals[:, 0]
    )
    input_grad = upstream_gradient + grad_back
    small_sums = jnp.stack(
        (g_gain1, g_gain2, g_gain3, g_shift1, g_shift2, g_shift3, g_out_bias), axis=0
    )
    bias_sums = g_hidden_bias.reshape(D, 4).T
    sums = jnp.concatenate([small_sums, bias_sums], axis=0)
    picks = jnp.eye(11, 256, dtype=jnp.bfloat16)
    attn_in_grad, attn_out_grad, small_grad = reduce(
        [(flat(normed1), flat(grad_qkv)), out_factors, (sums.astype(jnp.bfloat16), picks)]
    )
    return (
        layer_out,
        input_grad,
        memory_grad,
        attn_in_grad,
        attn_out_grad,
        cross_query_grad,
        cross_kv_grad,
        cross_out_grad,
        mlp_in_grad,
        mlp_out_grad,
        small_grad[:, :3],
        small_grad[:, 3:7],
        small_grad[:, 7:11].reshape(-1),
    )


def solution(mesh):
    in_specs = (
        P(("fsdp", "dp"), None, None),
        P(("fsdp", "dp"), None, None),
        P(("fsdp", "dp")),
        P(("fsdp", "dp"), None, None),
        P(("fsdp", "dp"), None),
        P(("fsdp", "dp"), None),
        P(("fsdp", "dp"), None),
        P(("fsdp", "dp"), None),
        P(("fsdp", "dp"), None),
        P(("fsdp", "dp"), None),
        P(("fsdp", "dp"), None),
        P(("fsdp", "dp"), None),
        P(("fsdp", "dp"), None),
        P(("fsdp", "dp")),
    )
    out_specs = (
        P(("fsdp", "dp"), None, None),
        P(("fsdp", "dp"), None, None),
        P(("fsdp", "dp"), None, None),
        P(("fsdp", "dp"), None),
        P(("fsdp", "dp"), None),
        P(("fsdp", "dp"), None),
        P(("fsdp", "dp"), None),
        P(("fsdp", "dp"), None),
        P(("fsdp", "dp"), None),
        P(("fsdp", "dp"), None),
        P(("fsdp", "dp"), None),
        P(("fsdp", "dp"), None),
        P(("fsdp", "dp")),
    )
    if dict(mesh.shape) == {"fsdp": 8, "dp": 4}:
        program = functools.partial(local, gather_grid, reduce_grid)
    else:
        program = functools.partial(local, gather_plain, reduce_plain)
    return jax.shard_map(program, mesh=mesh, in_specs=in_specs, out_specs=out_specs, check_vma=False)
```

```python
import functools

import jax
import jax.numpy as jnp
from jax import lax
from jax.experimental import pallas as pl
from jax.experimental.pallas import tpu as pltpu
from jax.sharding import PartitionSpec as P

D = 768
HEADS = 12
HEAD_DIM = 64
PREFIX = 32


EPS = 1e-05


def norm_forward(value_tensor, gain, shift):
    mean = jnp.mean(value_tensor, axis=-1, keepdims=True)
    centred = value_tensor - mean
    spread = jnp.mean(centred * centred, axis=-1, keepdims=True)
    scale_inv = lax.rsqrt(spread + EPS)
    standard = centred * scale_inv
    return (standard * gain + shift, standard, scale_inv)


def norm_backward(upstream_gradient, standard, scale_inv, gain):
    grad_gain = jnp.sum(upstream_gradient * standard, axis=0)
    grad_shift = jnp.sum(upstream_gradient, axis=0)
    inner = upstream_gradient * gain
    first = jnp.mean(inner, axis=-1, keepdims=True)
    second = jnp.mean(inner * standard, axis=-1, keepdims=True)
    return (scale_inv * (inner - first - standard * second), grad_gain, grad_shift)


def project(value_tensor, weight_matrix):
    return jnp.einsum("...h,ht->...t", value_tensor, weight_matrix, preferred_element_type=jnp.float32)


def back_project(upstream_gradient, weight_matrix):
    return jnp.einsum(
        "...j,aj->...a", upstream_gradient, weight_matrix, preferred_element_type=jnp.float32
    )


PAIRS = HEADS // 2
LANES = 2 * HEAD_DIM


def dot(a, b, over):
    return lax.dot_general(a, b, (over, ((), ())), preferred_element_type=jnp.float32)


NATURAL = ((1,), (0,))
BOTH_LAST = ((1,), (1,))
BOTH_FIRST = ((0,), (0,))


def low_lanes(rows):
    return lax.broadcasted_iota(jnp.int32, (rows, LANES), 1) < HEAD_DIM


def stacked(pair, level):
    low = low_lanes(pair.shape[0])
    first = jnp.where(low, level, 0.0).astype(jnp.bfloat16)
    second = jnp.where(low, 0.0, level).astype(jnp.bfloat16)
    return jnp.concatenate([pair * first, pair * second], axis=0)


def unstacked(value):
    rows = value.shape[0] // 2
    return jnp.where(low_lanes(rows), value[:rows], value[rows:])


def lanes_of(ref, start):
    return ref[0, :, start : start + LANES]


def forward_pair(query, key, value, allowed):
    scores = dot(key, stacked(query, HEAD_DIM**-0.5), BOTH_LAST)
    if allowed is not None:
        scores = jnp.where(allowed, scores, -1e30)
    weights = jnp.exp(scores - jnp.max(scores, axis=0, keepdims=True))
    probs = (weights * (1.0 / jnp.sum(weights, axis=0, keepdims=True))).astype(jnp.bfloat16)
    context = unstacked(dot(probs, value, BOTH_FIRST)).astype(jnp.bfloat16)
    return context, probs


def backward_pair(query, key, value, probs, grad):
    scale = HEAD_DIM**-0.5
    grads = stacked(grad, 1.0)
    grad_probs = dot(value, grads, BOTH_LAST)
    wide = probs.astype(jnp.float32)
    delta = jnp.sum(grad_probs * wide, axis=0, keepdims=True)
    grad_scores = (wide * (grad_probs - delta)).astype(jnp.bfloat16)
    grad_key = dot(grad_scores, stacked(query, scale), NATURAL).astype(jnp.bfloat16)
    grad_value = dot(probs, grads, NATURAL).astype(jnp.bfloat16)
    grad_query = (unstacked(dot(grad_scores, key, BOTH_FIRST)) * scale).astype(jnp.bfloat16)
    return grad_query, grad_key, grad_value


def self_forward_body(lens, qkv, context, probs):
    rows = qkv.shape[1]
    at_key = lax.broadcasted_iota(jnp.int32, (rows, 2 * rows), 0)
    at_query = lax.broadcasted_iota(jnp.int32, (rows, 2 * rows), 1)
    at_query = jnp.where(at_query < rows, at_query, at_query - rows)
    allowed = (at_key <= at_query) & (at_key < PREFIX + lens[pl.program_id(0)])
    for p in range(PAIRS):
        at = p * LANES
        out, kept = forward_pair(
            lanes_of(qkv, at), lanes_of(qkv, D + at), lanes_of(qkv, 2 * D + at), allowed
        )
        context[0, :, at : at + LANES] = out
        probs[0, p] = kept


def self_backward_body(qkv, probs, grad, grad_qkv):
    for p in range(PAIRS):
        at = p * LANES
        gq, gk, gv = backward_pair(
            lanes_of(qkv, at),
            lanes_of(qkv, D + at),
            lanes_of(qkv, 2 * D + at),
            probs[0, p],
            lanes_of(grad, at),
        )
        grad_qkv[0, :, at : at + LANES] = gq
        grad_qkv[0, :, D + at : D + at + LANES] = gk
        grad_qkv[0, :, 2 * D + at : 2 * D + at + LANES] = gv


def cross_forward_body(query, kv, context, probs):
    for p in range(PAIRS):
        at = p * LANES
        out, kept = forward_pair(lanes_of(query, at), lanes_of(kv, at), lanes_of(kv, D + at), None)
        context[0, :, at : at + LANES] = out
        probs[0, p] = kept


def cross_backward_body(query, kv, probs, grad, grad_query, grad_kv):
    for p in range(PAIRS):
        at = p * LANES
        gq, gk, gv = backward_pair(
            lanes_of(query, at),
            lanes_of(kv, at),
            lanes_of(kv, D + at),
            probs[0, p],
            lanes_of(grad, at),
        )
        grad_query[0, :, at : at + LANES] = gq
        grad_kv[0, :, at : at + LANES] = gk
        grad_kv[0, :, D + at : D + at + LANES] = gv


def whole_block(shape):
    rest = len(shape) - 1
    return pl.BlockSpec((1,) + tuple(shape[1:]), lambda s, *_: (s,) + (0,) * rest)


def per_sequence(body, name, inputs, shapes, lens=None):
    outs = [jax.ShapeDtypeStruct(shape, jnp.bfloat16) for shape in shapes]
    return pl.pallas_call(
        body,
        out_shape=outs,
        grid_spec=pltpu.PrefetchScalarGridSpec(
            num_scalar_prefetch=0 if lens is None else 1,
            grid=(inputs[0].shape[0],),
            in_specs=[whole_block(v.shape) for v in inputs],
            out_specs=[whole_block(shape) for shape in shapes],
        ),
        name=name,
    )(*(() if lens is None else (lens,)), *inputs)


def self_forward(qkv, lens):
    seqs, rows, _ = qkv.shape
    return per_sequence(
        self_forward_body,
        "self_forward",
        [qkv],
        [(seqs, rows, D), (seqs, PAIRS, rows, 2 * rows)],
        lens,
    )


def self_backward(qkv, probs, grad):
    return per_sequence(self_backward_body, "self_backward", [qkv, probs, grad], [qkv.shape])[0]


def cross_forward(query, kv):
    seqs, rows, _ = query.shape
    return per_sequence(
        cross_forward_body,
        "cross_forward",
        [query, kv],
        [query.shape, (seqs, PAIRS, kv.shape[1], 2 * rows)],
    )


def cross_backward(query, kv, probs, grad):
    return per_sequence(
        cross_backward_body,
        "cross_backward",
        [query, kv, probs, grad],
        [query.shape, kv.shape],
    )


AXES = ("fsdp", "dp")


def grid_rank(z, x, y, core):
    return ((z * 2 + x) * 2 + y) * 2 + core


def grid_perm(move):
    return [
        (grid_rank(z, x, y, core), grid_rank(*move(z, x, y, core)))
        for z in range(4)
        for x in range(2)
        for y in range(2)
        for core in range(2)
    ]


CORE = grid_perm(lambda z, x, y, core: (z, x, y, core ^ 1))
ZSHIFT = [
    grid_perm(lambda z, x, y, core, k=k: ((z + k) % 4, x, y, core)) for k in range(4)
]
FIRST = grid_perm(lambda z, x, y, core: (z, x ^ (1 - core), y ^ core, core))
SECOND = grid_perm(lambda z, x, y, core: (z, x ^ core, y ^ (1 - core), core))


def move(value, perm):
    return lax.ppermute(value, AXES, perm)


def place():
    outer, inner = lax.axis_index("fsdp"), lax.axis_index("dp")
    return outer // 2, outer % 2, inner // 2, inner % 2


def half_of(value, side):
    width = value.shape[-1] // 2
    return lax.dynamic_slice_in_dim(value, side * width, width, axis=-1)


def after(value, *earlier):
    return lax.optimization_barrier((value,) + earlier)[0]


def assemble_body(widths, spot, *refs):
    parts, outs = refs[:8], refs[8:]
    x, y, core = spot[1], spot[2], spot[3]
    for theirs in range(2):
        side = 1 - core if theirs else core
        for j in range(4):
            at_x = x ^ (0, 1 - side, side, 1)[j]
            at_y = y ^ (0, side, 1 - side, 1)[j]
            offset = 0
            for width, out in zip(widths, outs):
                out[0, at_x, at_y, side] = parts[theirs * 4 + j][0, :, offset : offset + width]
                offset += width


def assemble(parts, rows, widths, spot):
    outs = pl.pallas_call(
        functools.partial(assemble_body, widths),
        out_shape=[jax.ShapeDtypeStruct((4, 2, 2, 2, rows, w), jnp.bfloat16) for w in widths],
        grid_spec=pltpu.PrefetchScalarGridSpec(
            num_scalar_prefetch=1,
            grid=(4,),
            in_specs=[pl.BlockSpec((1, rows, sum(widths)), lambda k, spot: (k, 0, 0))] * 8,
            out_specs=[
                pl.BlockSpec(
                    (1, 2, 2, 2, rows, w),
                    lambda k, spot: (lax.rem(spot[0] + 4 - k, 4), 0, 0, 0, 0, 0),
                )
                for w in widths
            ],
        ),
        name="assemble",
    )(spot, *parts)
    return [o.reshape(32 * rows, w) for o, w in zip(outs, widths)]


class GridGather:
    def __init__(self):
        self.lines = ()
        self.crossed = ()

    def spread(self, shards):
        own = jnp.concatenate(shards, axis=1) if len(shards) > 1 else shards[0]
        own = after(own, *self.lines)
        self.lines = tuple(move(own, ZSHIFT[k]) for k in (1, 2, 3))
        return jnp.stack((own,) + self.lines)

    def cross(self, line, *earlier):
        ready = after(line, *self.crossed, *earlier)
        one = move(ready, FIRST)
        two = move(ready, SECOND)
        both = move(one, SECOND)
        self.crossed = (one, two) if earlier else (both,)
        parts = [line, one, two, both]
        return parts + [move(p, CORE) for p in parts]

    def join(self, parts, shards, *earlier):
        rows = shards[0].shape[0]
        widths = [s.shape[1] for s in shards]
        if earlier:
            parts = lax.optimization_barrier(tuple(parts) + earlier)[: len(parts)]
        return assemble(parts, rows, widths, jnp.stack(place()).astype(jnp.int32))


class PlainGather:
    def spread(self, shards):
        return None

    def cross(self, line, *earlier):
        return None

    def join(self, parts, shards, *earlier):
        widths = [s.shape[1] for s in shards]
        whole = lax.all_gather(jnp.concatenate(shards, axis=1), AXES, axis=0, tiled=True)
        results = []
        offset = 0
        for width in widths:
            results.append(whole[:, offset : offset + width])
            offset += width
        return results


def split_body(count, which, *refs):
    del which
    keeps, sends, outs = refs[: 2 * count], refs[2 * count : 4 * count], refs[4 * count :]
    for source, out in ((keeps, outs[0]), (sends, outs[1])):
        offset = 0
        for i in range(count):
            width = source[2 * i].shape[-1]
            total = source[2 * i][...].astype(jnp.float32) + source[2 * i + 1][...].astype(
                jnp.float32
            )
            out[:, :, :, offset : offset + width] = total.astype(jnp.bfloat16)
            offset += width


def split_add(pairs, rows):
    z, x, y, core = place()
    first = jnp.where(core == 0, x, y)
    second = jnp.where(core == 0, y, x)
    first_weight = jnp.where(core == 0, 2, 1)
    second_weight = 3 - first_weight
    which = jnp.stack(
        [
            (first ^ f) * first_weight + (second ^ s) * second_weight
            for s in range(2)
            for f in range(2)
        ]
    ).astype(jnp.int32)
    views, keep_specs, send_specs = [], [], []
    for keep, got in pairs:
        width = keep.shape[1]
        block = (4, 1, 2 * rows, width)
        for value in (keep, got):
            views.append(value.reshape(4, 4, 2 * rows, width))
            keep_specs.append(pl.BlockSpec(block, lambda f, which: (0, which[f], 0, 0)))
            send_specs.append(pl.BlockSpec(block, lambda f, which: (0, which[2 + f], 0, 0)))
    total = sum(keep.shape[1] for keep, _ in pairs)
    shape = jax.ShapeDtypeStruct((4, 2, 2 * rows, total), jnp.bfloat16)
    out_spec = pl.BlockSpec((4, 1, 2 * rows, total), lambda f, which: (0, f, 0, 0))
    return pl.pallas_call(
        functools.partial(split_body, len(pairs)),
        out_shape=[shape, shape],
        grid_spec=pltpu.PrefetchScalarGridSpec(
            num_scalar_prefetch=1,
            grid=(2,),
            in_specs=keep_specs + send_specs,
            out_specs=[out_spec, out_spec],
        ),
        name="split_add",
    )(which, *views, *views)


class GridReduction:
    def __init__(self, factors):
        core = place()[3]
        self.rows = factors[0][0].shape[-1] // 32
        self.sends = [contract_low(v, half_of(u, 1 - core)) for v, u in factors]
        self.factors = factors
        self.stage = 0

    def step(self):
        self.stage += 1
        return getattr(self, "hop%d" % self.stage)()

    def hop1(self):
        core = place()[3]
        self.got = [move(send, CORE) for send in self.sends]
        self.keeps = [contract_low(v, half_of(u, core)) for v, u in self.factors]
        return self.got

    def hop2(self):
        self.keep, send = split_add(list(zip(self.keeps, self.got)), self.rows)
        self.got = move(send, SECOND)
        return [self.got]

    def hop3(self):
        f32 = jnp.float32
        total = self.keep[:, 1].astype(f32) + self.got[:, 1].astype(f32)
        self.got_first = move(total.astype(jnp.bfloat16), FIRST)
        return [self.got_first]

    def hop4(self):
        z = place()[0]
        f32 = jnp.float32

        def plane(k):
            at = (z + k) % 4
            pick = lambda v: lax.dynamic_index_in_dim(v, at, 0, keepdims=False).astype(f32)
            return pick(self.keep[:, 0]) + pick(self.got[:, 0]) + pick(self.got_first)

        self.own = plane(0)
        self.planes = [move(plane(k).astype(jnp.bfloat16), ZSHIFT[k]) for k in (1, 2, 3)]
        return self.planes

    def results(self):
        while self.stage < 4:
            self.step()
        core, rows = place()[3], self.rows
        total = self.own + sum(p.astype(jnp.float32) for p in self.planes)
        mine = lax.dynamic_slice_in_dim(total, core * rows, rows, axis=0)
        other = move(lax.dynamic_slice_in_dim(total, (1 - core) * rows, rows, axis=0), CORE)
        left = jnp.where(core == 0, mine, other)
        right = jnp.where(core == 0, other, mine)
        results = []
        offset = 0
        for keep in self.keeps:
            width = keep.shape[1]
            results.append(
                jnp.concatenate(
                    [left[:, offset : offset + width], right[:, offset : offset + width]], axis=1
                )
            )
            offset += width
        return results


class PlainReduction:
    def __init__(self, factors):
        self.factors = factors
        self.sends = []

    def step(self):
        return []

    def results(self):
        packed = jnp.concatenate([contract_low(v, u) for v, u in self.factors], axis=1)
        summed = lax.psum_scatter(packed, AXES, scatter_dimension=0, tiled=True)
        summed = summed.astype(jnp.float32)
        results = []
        offset = 0
        for _, u in self.factors:
            results.append(summed[:, offset : offset + u.shape[-1]])
            offset += u.shape[-1]
        return results


def contract_low(value, upstream_gradient):
    over = tuple(range(value.ndim - 1))
    return lax.dot_general(
        value,
        upstream_gradient,
        ((over, over), ((), ())),
        preferred_element_type=jnp.float32,
    ).astype(jnp.bfloat16)


def local(
    gathering,
    reduction,
    tokens,
    memory,
    suffix_len,
    cotangent,
    attn_in,
    attn_out,
    cross_query,
    cross_kv,
    cross_out,
    mlp_in,
    mlp_out,
    ln_gain,
    shifts,
    mlp_bias,
):
    owned = attn_in.shape[0]
    small = jnp.concatenate(
        [
            ln_gain,
            shifts,
            mlp_bias.reshape(owned, 4),
            jnp.zeros((owned, 256 - 11), jnp.bfloat16),
        ],
        axis=1,
    )
    gather = gathering()
    first, second, third, fourth = (
        [attn_in, small],
        [attn_out, cross_query, cross_kv, cross_out],
        [mlp_in],
        [mlp_out],
    )
    lines = [gather.spread(shards) for shards in (first, second, third, fourth)]
    first_parts = gather.cross(lines[0])
    second_parts = gather.cross(lines[1])
    w_qkv, smalls = gather.join(first_parts, first)
    gains, biases, hidden_bias = smalls[:, :3], smalls[:, 3:7], smalls[:, 7:11].reshape(-1)
    seqs, rows, width = tokens.shape
    low = lambda v: v.astype(jnp.bfloat16)
    flat = lambda v: v.reshape(seqs * rows, v.shape[-1])
    by_seq = lambda v: v.reshape(seqs, rows, v.shape[-1])
    live = jnp.arange(rows)[None, :] < (PREFIX + suffix_len)[:, None]
    gain_vals = gains.astype(jnp.float32)
    bias_vals = biases.astype(jnp.float32)
    stream0 = flat(tokens).astype(jnp.float32)
    normed1, standard1, inverse1 = norm_forward(stream0, gain_vals[:, 0], bias_vals[:, 0])
    normed1 = low(normed1)
    qkv = by_seq(low(project(normed1, w_qkv)))
    context, probs = self_forward(qkv, suffix_len)
    third_parts = gather.cross(lines[2], context)
    w_out, w_cquery, w_ckv, w_cout = gather.join(second_parts, second, context)
    context = flat(context)
    stream1 = stream0 + project(context, w_out)
    normed2, standard2, inverse2 = norm_forward(stream1, gain_vals[:, 1], bias_vals[:, 1])
    normed2 = low(normed2)
    cquery = by_seq(low(project(normed2, w_cquery)))
    ckv = low(project(memory, w_ckv))
    fourth_parts = gather.cross(lines[3], cquery)
    ccontext, cprobs = cross_forward(cquery, ckv)
    (w_in,) = gather.join(third_parts, third, ccontext)
    ccontext = flat(ccontext)
    stream2 = stream1 + project(ccontext, w_cout)
    normed3, standard3, inverse3 = norm_forward(stream2, gain_vals[:, 2], bias_vals[:, 2])
    normed3 = low(normed3)
    pre = project(normed3, w_in) + hidden_bias.astype(jnp.float32)
    activated, gelu_back = jax.vjp(lambda v: jax.nn.gelu(v, approximate=True), pre)
    activated = low(activated)
    (w_down,) = gather.join(fourth_parts, fourth, activated)
    layer_out = by_seq(low(stream2 + project(activated, w_down) + bias_vals[:, 3]))

    upstream = flat(cotangent.astype(jnp.float32) * live[..., None].astype(jnp.float32))
    dout3 = low(upstream)
    down_sum = reduction([(activated, dout3)])
    g_out_bias = jnp.sum(dout3, axis=0, dtype=jnp.float32)
    grad_act = back_project(after(dout3, *down_sum.sends), w_down)
    dpre = low(gelu_back(grad_act)[0])
    g_hidden_bias = jnp.sum(dpre, axis=0, dtype=jnp.float32)
    in_sum = reduction([(normed3, dpre)])
    dpre = after(dpre, *down_sum.step(), *in_sum.sends)
    grad_back, g_gain3, g_shift3 = norm_backward(
        back_project(dpre, w_in), standard3, inverse3, gain_vals[:, 2]
    )
    upstream = upstream + grad_back
    dout2 = low(upstream)
    dccontext = by_seq(low(back_project(dout2, w_cout)))
    dccontext = after(dccontext, *down_sum.step(), *in_sum.step())
    dcquery, dckv = cross_backward(cquery, ckv, cprobs, dccontext)
    dcq = flat(dcquery)
    cross_sum = reduction([(normed2, dcq), (memory, dckv), (ccontext, dout2)])
    dcq = after(dcq, *down_sum.step(), *in_sum.step(), *cross_sum.sends)
    grad_back, g_gain2, g_shift2 = norm_backward(
        back_project(dcq, w_cquery), standard2, inverse2, gain_vals[:, 1]
    )
    upstream = upstream + grad_back
    dout1 = low(upstream)
    dcontext = by_seq(low(back_project(dout1, w_out)))
    dcontext = after(dcontext, *down_sum.step(), *in_sum.step(), *cross_sum.step())
    dqkv = flat(self_backward(qkv, probs, dcontext))
    grad_back, g_gain1, g_shift1 = norm_backward(
        back_project(dqkv, w_qkv), standard1, inverse1, gain_vals[:, 0]
    )
    input_grad = by_seq(upstream + grad_back)
    small_sums = jnp.stack(
        (g_gain1, g_gain2, g_gain3, g_shift1, g_shift2, g_shift3, g_out_bias), axis=0
    )
    bias_sums = g_hidden_bias.reshape(D, 4).T
    sums = jnp.concatenate([small_sums, bias_sums], axis=0)
    picks = jnp.eye(11, 256, dtype=jnp.bfloat16)
    attn_sum = reduction([(normed1, dqkv), (context, dout1), (low(sums), picks)])
    memory_grad = back_project(after(dckv, *attn_sum.sends), w_ckv)
    (mlp_out_grad,) = down_sum.results()
    (mlp_in_grad,) = in_sum.results()
    cross_query_grad, cross_kv_grad, cross_out_grad = cross_sum.results()
    attn_in_grad, attn_out_grad, small_grad = attn_sum.results()
    return (
        layer_out,
        input_grad,
        memory_grad,
        attn_in_grad,
        attn_out_grad,
        cross_query_grad,
        cross_kv_grad,
        cross_out_grad,
        mlp_in_grad,
        mlp_out_grad,
        small_grad[:, :3],
        small_grad[:, 3:7],
        small_grad[:, 7:11].reshape(-1),
    )


def solution(mesh):
    in_specs = (
        P(("fsdp", "dp"), None, None),
        P(("fsdp", "dp"), None, None),
        P(("fsdp", "dp")),
        P(("fsdp", "dp"), None, None),
        P(("fsdp", "dp"), None),
        P(("fsdp", "dp"), None),
        P(("fsdp", "dp"), None),
        P(("fsdp", "dp"), None),
        P(("fsdp", "dp"), None),
        P(("fsdp", "dp"), None),
        P(("fsdp", "dp"), None),
        P(("fsdp", "dp"), None),
        P(("fsdp", "dp"), None),
        P(("fsdp", "dp")),
    )
    out_specs = (
        P(("fsdp", "dp"), None, None),
        P(("fsdp", "dp"), None, None),
        P(("fsdp", "dp"), None, None),
        P(("fsdp", "dp"), None),
        P(("fsdp", "dp"), None),
        P(("fsdp", "dp"), None),
        P(("fsdp", "dp"), None),
        P(("fsdp", "dp"), None),
        P(("fsdp", "dp"), None),
        P(("fsdp", "dp"), None),
        P(("fsdp", "dp"), None),
        P(("fsdp", "dp"), None),
        P(("fsdp", "dp")),
    )
    if dict(mesh.shape) == {"fsdp": 8, "dp": 4}:
        program = functools.partial(local, GridGather, GridReduction)
    else:
        program = functools.partial(local, PlainGather, PlainReduction)
    return jax.shard_map(program, mesh=mesh, in_specs=in_specs, out_specs=out_specs, check_vma=False)
```

```python
import functools

import jax
import jax.numpy as jnp
from jax import lax
from jax.experimental import pallas as pl
from jax.experimental.pallas import tpu as pltpu
from jax.sharding import PartitionSpec as P

D = 768
HEADS = 12
HEAD_DIM = 64
PREFIX = 32


EPS = 1e-05


def norm_forward(value_tensor, gain, shift):
    mean = jnp.mean(value_tensor, axis=-1, keepdims=True)
    centred = value_tensor - mean
    spread = jnp.mean(centred * centred, axis=-1, keepdims=True)
    scale_inv = lax.rsqrt(spread + EPS)
    standard = centred * scale_inv
    return (standard * gain + shift, standard, scale_inv)


def norm_backward(upstream_gradient, standard, scale_inv, gain):
    grad_gain = jnp.sum(upstream_gradient * standard, axis=0)
    grad_shift = jnp.sum(upstream_gradient, axis=0)
    inner = upstream_gradient * gain
    first = jnp.mean(inner, axis=-1, keepdims=True)
    second = jnp.mean(inner * standard, axis=-1, keepdims=True)
    return (scale_inv * (inner - first - standard * second), grad_gain, grad_shift)


def project(value_tensor, weight_matrix):
    return jnp.einsum("...h,ht->...t", value_tensor, weight_matrix, preferred_element_type=jnp.float32)


def back_project(upstream_gradient, weight_matrix):
    return jnp.einsum(
        "...j,aj->...a", upstream_gradient, weight_matrix, preferred_element_type=jnp.float32
    )


PAIRS = HEADS // 2
LANES = 2 * HEAD_DIM


def dot(a, b, over):
    return lax.dot_general(a, b, (over, ((), ())), preferred_element_type=jnp.float32)


NATURAL = ((1,), (0,))
BOTH_LAST = ((1,), (1,))
BOTH_FIRST = ((0,), (0,))


def low_lanes(rows):
    return lax.broadcasted_iota(jnp.int32, (rows, LANES), 1) < HEAD_DIM


def stacked(pair, level):
    low = low_lanes(pair.shape[0])
    first = jnp.where(low, level, 0.0).astype(jnp.bfloat16)
    second = jnp.where(low, 0.0, level).astype(jnp.bfloat16)
    return jnp.concatenate([pair * first, pair * second], axis=0)


def unstacked(value):
    rows = value.shape[0] // 2
    return jnp.where(low_lanes(rows), value[:rows], value[rows:])


def lanes_of(ref, start):
    return ref[0, :, start : start + LANES]


def forward_pair(query, key, value, allowed):
    scores = dot(key, stacked(query, HEAD_DIM**-0.5), BOTH_LAST)
    if allowed is not None:
        scores = jnp.where(allowed, scores, -1e30)
    weights = jnp.exp(scores - jnp.max(scores, axis=0, keepdims=True))
    probs = (weights * (1.0 / jnp.sum(weights, axis=0, keepdims=True))).astype(jnp.bfloat16)
    context = unstacked(dot(probs, value, BOTH_FIRST)).astype(jnp.bfloat16)
    return context, probs


def backward_pair(query, key, value, probs, grad):
    scale = HEAD_DIM**-0.5
    grads = stacked(grad, 1.0)
    grad_probs = dot(value, grads, BOTH_LAST)
    wide = probs.astype(jnp.float32)
    delta = jnp.sum(grad_probs * wide, axis=0, keepdims=True)
    grad_scores = (wide * (grad_probs - delta)).astype(jnp.bfloat16)
    grad_key = dot(grad_scores, stacked(query, scale), NATURAL).astype(jnp.bfloat16)
    grad_value = dot(probs, grads, NATURAL).astype(jnp.bfloat16)
    grad_query = (unstacked(dot(grad_scores, key, BOTH_FIRST)) * scale).astype(jnp.bfloat16)
    return grad_query, grad_key, grad_value


def self_forward_body(lens, qkv, context, probs):
    rows = qkv.shape[1]
    at_key = lax.broadcasted_iota(jnp.int32, (rows, 2 * rows), 0)
    at_query = lax.broadcasted_iota(jnp.int32, (rows, 2 * rows), 1)
    at_query = jnp.where(at_query < rows, at_query, at_query - rows)
    allowed = (at_key <= at_query) & (at_key < PREFIX + lens[pl.program_id(0)])
    for p in range(PAIRS):
        at = p * LANES
        out, kept = forward_pair(
            lanes_of(qkv, at), lanes_of(qkv, D + at), lanes_of(qkv, 2 * D + at), allowed
        )
        context[0, :, at : at + LANES] = out
        probs[0, p] = kept


def self_backward_body(qkv, probs, grad, grad_qkv):
    for p in range(PAIRS):
        at = p * LANES
        gq, gk, gv = backward_pair(
            lanes_of(qkv, at),
            lanes_of(qkv, D + at),
            lanes_of(qkv, 2 * D + at),
            probs[0, p],
            lanes_of(grad, at),
        )
        grad_qkv[0, :, at : at + LANES] = gq
        grad_qkv[0, :, D + at : D + at + LANES] = gk
        grad_qkv[0, :, 2 * D + at : 2 * D + at + LANES] = gv


def cross_forward_body(query, kv, context, probs):
    for p in range(PAIRS):
        at = p * LANES
        out, kept = forward_pair(lanes_of(query, at), lanes_of(kv, at), lanes_of(kv, D + at), None)
        context[0, :, at : at + LANES] = out
        probs[0, p] = kept


def cross_backward_body(query, kv, probs, grad, grad_query, grad_kv):
    for p in range(PAIRS):
        at = p * LANES
        gq, gk, gv = backward_pair(
            lanes_of(query, at),
            lanes_of(kv, at),
            lanes_of(kv, D + at),
            probs[0, p],
            lanes_of(grad, at),
        )
        grad_query[0, :, at : at + LANES] = gq
        grad_kv[0, :, at : at + LANES] = gk
        grad_kv[0, :, D + at : D + at + LANES] = gv


def whole_block(shape):
    rest = len(shape) - 1
    return pl.BlockSpec((1,) + tuple(shape[1:]), lambda s, *_: (s,) + (0,) * rest)


def per_sequence(body, name, inputs, shapes, lens=None):
    outs = [jax.ShapeDtypeStruct(shape, jnp.bfloat16) for shape in shapes]
    return pl.pallas_call(
        body,
        out_shape=outs,
        grid_spec=pltpu.PrefetchScalarGridSpec(
            num_scalar_prefetch=0 if lens is None else 1,
            grid=(inputs[0].shape[0],),
            in_specs=[whole_block(v.shape) for v in inputs],
            out_specs=[whole_block(shape) for shape in shapes],
        ),
        name=name,
    )(*(() if lens is None else (lens,)), *inputs)


def self_forward(qkv, lens):
    seqs, rows, _ = qkv.shape
    return per_sequence(
        self_forward_body,
        "self_forward",
        [qkv],
        [(seqs, rows, D), (seqs, PAIRS, rows, 2 * rows)],
        lens,
    )


def self_backward(qkv, probs, grad):
    return per_sequence(self_backward_body, "self_backward", [qkv, probs, grad], [qkv.shape])[0]


def cross_forward(query, kv):
    seqs, rows, _ = query.shape
    return per_sequence(
        cross_forward_body,
        "cross_forward",
        [query, kv],
        [query.shape, (seqs, PAIRS, kv.shape[1], 2 * rows)],
    )


def cross_backward(query, kv, probs, grad):
    return per_sequence(
        cross_backward_body,
        "cross_backward",
        [query, kv, probs, grad],
        [query.shape, kv.shape],
    )


AXES = ("fsdp", "dp")


def grid_rank(z, x, y, core):
    return ((z * 2 + x) * 2 + y) * 2 + core


def grid_perm(move):
    return [
        (grid_rank(z, x, y, core), grid_rank(*move(z, x, y, core)))
        for z in range(4)
        for x in range(2)
        for y in range(2)
        for core in range(2)
    ]


CORE = grid_perm(lambda z, x, y, core: (z, x, y, core ^ 1))
ZNEAR = grid_perm(lambda z, x, y, core: (z ^ 1, x, y, core))
ZFAR = grid_perm(lambda z, x, y, core: (z ^ 2, x, y, core))
FIRST = grid_perm(lambda z, x, y, core: (z, x ^ (1 - core), y ^ core, core))
SECOND = grid_perm(lambda z, x, y, core: (z, x ^ core, y ^ (1 - core), core))


def move(value, perm):
    return lax.ppermute(value, AXES, perm)


def place():
    outer, inner = lax.axis_index("fsdp"), lax.axis_index("dp")
    return outer // 2, outer % 2, inner // 2, inner % 2


def half_of(value, side):
    width = value.shape[-1] // 2
    return lax.dynamic_slice_in_dim(value, side * width, width, axis=-1)


def after(value, *earlier):
    return lax.optimization_barrier((value,) + earlier)[0]


def assemble_body(widths, spot, *refs):
    parts, outs = refs[:8], refs[8:]
    x, y, core = spot[1], spot[2], spot[3]
    for theirs in range(2):
        side = 1 - core if theirs else core
        for j in range(4):
            at_x = x ^ (0, 1 - side, side, 1)[j]
            at_y = y ^ (0, side, 1 - side, 1)[j]
            offset = 0
            for width, out in zip(widths, outs):
                out[0, at_x, at_y, side] = parts[theirs * 4 + j][0, :, offset : offset + width]
                offset += width


def assemble(parts, rows, widths, spot):
    outs = pl.pallas_call(
        functools.partial(assemble_body, widths),
        out_shape=[jax.ShapeDtypeStruct((4, 2, 2, 2, rows, w), jnp.bfloat16) for w in widths],
        grid_spec=pltpu.PrefetchScalarGridSpec(
            num_scalar_prefetch=1,
            grid=(4,),
            in_specs=[pl.BlockSpec((1, rows, sum(widths)), lambda k, spot: (k, 0, 0))] * 8,
            out_specs=[
                pl.BlockSpec(
                    (1, 2, 2, 2, rows, w),
                    lambda k, spot: (spot[0] ^ (2 * lax.rem(k, 2) + k // 2), 0, 0, 0, 0, 0),
                )
                for w in widths
            ],
        ),
        name="assemble",
    )(spot, *parts)
    return [o.reshape(32 * rows, w) for o, w in zip(outs, widths)]


class GridGather:
    def __init__(self, shards):
        self.shards = shards
        self.own = jnp.concatenate(shards, axis=1) if len(shards) > 1 else shards[0]

    def spread(self, *earlier):
        own = after(self.own, *earlier)
        self.two = jnp.stack((self.own, move(own, ZFAR)))
        self.along = (move(self.two, ZNEAR),)
        return self.along

    def cross(self, *earlier):
        self.line = jnp.concatenate((self.two,) + self.along)
        ready = after(self.line, *earlier)
        self.sides = (move(ready, FIRST), move(ready, SECOND))
        return self.sides

    def corner(self, *earlier):
        self.both = (move(after(self.sides[0], *earlier), SECOND),)
        return self.both

    def swap(self):
        parts = (self.line,) + self.sides + self.both
        self.parts = parts + tuple(move(p, CORE) for p in parts)
        return self.parts

    def join(self, *earlier):
        parts = self.parts
        if earlier:
            parts = lax.optimization_barrier(parts + earlier)[: len(parts)]
        rows = self.shards[0].shape[0]
        widths = [s.shape[1] for s in self.shards]
        return assemble(parts, rows, widths, jnp.stack(place()).astype(jnp.int32))


class PlainGather:
    def __init__(self, shards):
        self.shards = shards

    along = ()

    def spread(self, *earlier):
        return ()

    cross = corner = spread

    def swap(self):
        return ()

    def join(self, *earlier):
        widths = [s.shape[1] for s in self.shards]
        whole = lax.all_gather(jnp.concatenate(self.shards, axis=1), AXES, axis=0, tiled=True)
        results = []
        offset = 0
        for width in widths:
            results.append(whole[:, offset : offset + width])
            offset += width
        return results


def split_body(count, which, *refs):
    del which
    keeps, sends, outs = refs[: 2 * count], refs[2 * count : 4 * count], refs[4 * count :]
    for source, out in ((keeps, outs[0]), (sends, outs[1])):
        offset = 0
        for i in range(count):
            width = source[2 * i].shape[-1]
            total = source[2 * i][...].astype(jnp.float32) + source[2 * i + 1][...].astype(
                jnp.float32
            )
            out[:, :, :, offset : offset + width] = total.astype(jnp.bfloat16)
            offset += width


def split_add(pairs, rows):
    z, x, y, core = place()
    first = jnp.where(core == 0, x, y)
    second = jnp.where(core == 0, y, x)
    first_weight = jnp.where(core == 0, 2, 1)
    second_weight = 3 - first_weight
    which = jnp.stack(
        [
            (first ^ f) * first_weight + (second ^ s) * second_weight
            for s in range(2)
            for f in range(2)
        ]
    ).astype(jnp.int32)
    views, keep_specs, send_specs = [], [], []
    for keep, got in pairs:
        width = keep.shape[1]
        block = (4, 1, 2 * rows, width)
        for value in (keep, got):
            views.append(value.reshape(4, 4, 2 * rows, width))
            keep_specs.append(pl.BlockSpec(block, lambda f, which: (0, which[f], 0, 0)))
            send_specs.append(pl.BlockSpec(block, lambda f, which: (0, which[2 + f], 0, 0)))
    total = sum(keep.shape[1] for keep, _ in pairs)
    shape = jax.ShapeDtypeStruct((4, 2, 2 * rows, total), jnp.bfloat16)
    out_spec = pl.BlockSpec((4, 1, 2 * rows, total), lambda f, which: (0, f, 0, 0))
    return pl.pallas_call(
        functools.partial(split_body, len(pairs)),
        out_shape=[shape, shape],
        grid_spec=pltpu.PrefetchScalarGridSpec(
            num_scalar_prefetch=1,
            grid=(2,),
            in_specs=keep_specs + send_specs,
            out_specs=[out_spec, out_spec],
        ),
        name="split_add",
    )(which, *views, *views)


def summed(partial):
    return lax.psum_scatter(partial, AXES, scatter_dimension=0, tiled=True)


class GridReduction:
    def __init__(self, factors):
        core = place()[3]
        self.rows = factors[0][0].shape[-1] // 32
        self.sends = [contract_low(v, half_of(u, 1 - core)) for v, u in factors]
        self.factors = factors
        self.stage = 0

    def add(self, value, upstream_gradient):
        side = 1 - place()[3]
        self.sends.append(contract_low(value, half_of(upstream_gradient, side)))
        self.factors.append((value, upstream_gradient))

    def step(self, *earlier):
        self.stage += 1
        return getattr(self, "hop%d" % self.stage)(*earlier)

    def hop1(self):
        core = place()[3]
        self.got = [move(send, CORE) for send in self.sends]
        self.keeps = [contract_low(v, half_of(u, core)) for v, u in self.factors]
        return self.got

    def hop2(self, *earlier):
        keeps = [after(self.keeps[0], *earlier)] + self.keeps[1:]
        self.keep, send = split_add(list(zip(keeps, self.got)), self.rows)
        self.got = move(send, SECOND)
        return [self.got]

    def hop3(self, *earlier):
        f32 = jnp.float32
        self.got = after(self.got, *earlier)
        total = self.keep[:, 1].astype(f32) + self.got[:, 1].astype(f32)
        self.half = total.astype(jnp.bfloat16)
        self.got_first = move(self.half, FIRST)
        return [self.got_first]

    def hop4(self, *earlier):
        z = place()[0]
        self.got_first = after(self.got_first, *earlier)
        f32 = jnp.float32

        def plane(k):
            at = z ^ k
            pick = lambda v: lax.dynamic_index_in_dim(v, at, 0, keepdims=False).astype(f32)
            return pick(self.keep[:, 0]) + pick(self.got[:, 0]) + pick(self.got_first)

        self.own, self.far = plane(0), plane(2)
        self.near = move(jnp.stack([plane(1), plane(3)]).astype(jnp.bfloat16), ZNEAR)
        return [self.near]

    def hop5(self, *earlier):
        near = after(self.near, *earlier).astype(jnp.float32)
        self.own = self.own + near[0]
        self.last = move((self.far + near[1]).astype(jnp.bfloat16), ZFAR)
        return [self.last]

    def results(self):
        while self.stage < 5:
            self.step()
        core, rows = place()[3], self.rows
        total = self.own + self.last.astype(jnp.float32)
        mine = lax.dynamic_slice_in_dim(total, core * rows, rows, axis=0)
        other = move(lax.dynamic_slice_in_dim(total, (1 - core) * rows, rows, axis=0), CORE)
        left = jnp.where(core == 0, mine, other)
        right = jnp.where(core == 0, other, mine)
        results = []
        offset = 0
        for keep in self.keeps:
            width = keep.shape[1]
            results.append(
                jnp.concatenate(
                    [left[:, offset : offset + width], right[:, offset : offset + width]], axis=1
                )
            )
            offset += width
        return results


class PlainReduction:
    def __init__(self, factors):
        self.factors = factors
        self.sends = []
        self.keep = self.half = self.got_first = self.own = jnp.zeros((), jnp.bfloat16)

    def add(self, value, upstream_gradient):
        self.factors.append((value, upstream_gradient))

    def step(self, *earlier):
        return []

    def results(self):
        packed = jnp.concatenate([contract_low(v, u) for v, u in self.factors], axis=1)
        total = summed(packed).astype(jnp.float32)
        results = []
        offset = 0
        for _, u in self.factors:
            results.append(total[:, offset : offset + u.shape[-1]])
            offset += u.shape[-1]
        return results


def contract_low(value, upstream_gradient):
    over = tuple(range(value.ndim - 1))
    return lax.dot_general(
        value,
        upstream_gradient,
        ((over, over), ((), ())),
        preferred_element_type=jnp.float32,
    ).astype(jnp.bfloat16)


def local(
    gathering,
    reduction,
    tokens,
    memory,
    suffix_len,
    cotangent,
    attn_in,
    attn_out,
    cross_query,
    cross_kv,
    cross_out,
    mlp_in,
    mlp_out,
    ln_gain,
    shifts,
    mlp_bias,
):
    owned = attn_in.shape[0]
    small = jnp.concatenate(
        [
            ln_gain,
            shifts,
            mlp_bias.reshape(owned, 4),
            jnp.zeros((owned, 256 - 11), jnp.bfloat16),
        ],
        axis=1,
    )
    first = gathering([attn_in, small])
    third = gathering([mlp_in])
    whole = lambda v: lax.all_gather(v, AXES, axis=0, tiled=True)
    w_second = whole(jnp.concatenate([attn_out, cross_query, cross_kv, cross_out], axis=1))
    fourth = gathering([mlp_out])
    third.spread(*first.spread())
    first.cross()
    third.cross(*first.corner())
    fourth.spread(*first.swap(), *third.along)
    w_qkv, smalls = first.join()
    gains, biases, hidden_bias = smalls[:, :3], smalls[:, 3:7], smalls[:, 7:11].reshape(-1)
    seqs, rows, width = tokens.shape
    low = lambda v: v.astype(jnp.bfloat16)
    flat = lambda v: v.reshape(seqs * rows, v.shape[-1])
    by_seq = lambda v: v.reshape(seqs, rows, v.shape[-1])
    live = jnp.arange(rows)[None, :] < (PREFIX + suffix_len)[:, None]
    gain_vals = gains.astype(jnp.float32)
    bias_vals = biases.astype(jnp.float32)
    stream0 = flat(tokens).astype(jnp.float32)
    normed1, standard1, inverse1 = norm_forward(stream0, gain_vals[:, 0], bias_vals[:, 0])
    normed1 = low(normed1)
    qkv = by_seq(low(project(normed1, w_qkv)))
    context, probs = self_forward(qkv, suffix_len)
    third.corner(context)
    third.swap()
    w_out, w_cquery = w_second[:, :D], w_second[:, D : 2 * D]
    w_ckv, w_cout = w_second[:, 2 * D : 4 * D], w_second[:, 4 * D :]
    context = flat(context)
    stream1 = stream0 + project(context, w_out)
    normed2, standard2, inverse2 = norm_forward(stream1, gain_vals[:, 1], bias_vals[:, 1])
    normed2 = low(normed2)
    cquery = by_seq(low(project(normed2, w_cquery)))
    ckv = low(project(memory, w_ckv))
    fourth.cross(cquery)
    ccontext, cprobs = cross_forward(cquery, ckv)
    ccontext = flat(ccontext)
    stream2 = stream1 + project(ccontext, w_cout)
    normed3, standard3, inverse3 = norm_forward(stream2, gain_vals[:, 2], bias_vals[:, 2])
    normed3 = low(normed3)
    (w_in,) = third.join(ccontext)
    fourth.corner(ccontext)
    fourth.swap()
    pre = project(normed3, w_in) + hidden_bias.astype(jnp.float32)
    activated, gelu_back = jax.vjp(lambda v: jax.nn.gelu(v, approximate=True), pre)
    activated = low(activated)

    upstream = flat(cotangent.astype(jnp.float32) * live[..., None].astype(jnp.float32))
    dout3 = low(upstream)
    down_partial = contract_low(activated, dout3)
    mlp_out_sum = summed(down_partial)
    g_out_bias = jnp.sum(dout3, axis=0, dtype=jnp.float32)
    (w_down,) = fourth.join(down_partial)
    grad_act = back_project(dout3, w_down)
    dpre = low(gelu_back(grad_act)[0])
    g_hidden_bias = jnp.sum(dpre, axis=0, dtype=jnp.float32)
    in_sum = reduction([(normed3, dpre)])
    dpre = after(dpre, *in_sum.sends)
    grad_back, g_gain3, g_shift3 = norm_backward(
        back_project(dpre, w_in), standard3, inverse3, gain_vals[:, 2]
    )
    upstream = upstream + grad_back
    dout2 = low(upstream)
    dccontext = by_seq(low(back_project(dout2, w_cout)))
    in_sum.step()
    arriving = in_sum.step()
    dccontext = after(dccontext, in_sum.keep)
    dcquery, dckv = cross_backward(cquery, ckv, cprobs, dccontext)
    dcq = flat(dcquery)
    grad_back, g_gain2, g_shift2 = norm_backward(
        back_project(dcq, w_cquery), standard2, inverse2, gain_vals[:, 1]
    )
    upstream = upstream + grad_back
    dout1 = low(upstream)
    cross_sum = reduction(
        [(normed2, dcq), (memory, dckv), (ccontext, dout2), (context, dout1)]
    )
    dcontext = by_seq(low(back_project(dout1, w_out)))
    dcontext = after(dcontext, *cross_sum.sends)
    dqkv = flat(self_backward(qkv, probs, dcontext))
    dqkv = after(dqkv, *arriving, *cross_sum.step())
    in_sum.step(dqkv)
    in_sum.step()
    in_sum.step()
    attn_sum = reduction([(normed1, dqkv)])
    grad_back, g_gain1, g_shift1 = norm_backward(
        back_project(after(dqkv, *attn_sum.sends), w_qkv),
        standard1,
        inverse1,
        gain_vals[:, 0],
    )
    input_grad = by_seq(upstream + grad_back)
    small_sums = jnp.stack(
        (g_gain1, g_gain2, g_gain3, g_shift1, g_shift2, g_shift3, g_out_bias), axis=0
    )
    bias_sums = g_hidden_bias.reshape(D, 4).T
    sums = jnp.concatenate([small_sums, bias_sums], axis=0)
    picks = jnp.eye(11, 256, dtype=jnp.bfloat16)
    attn_sum.add(low(sums), picks)
    attn_sum.step()
    cross_sum.step()
    cross_sum.step()
    arrived = attn_sum.step(cross_sum.half)
    attn_sum.step()
    memory_grad = back_project(after(dckv, *arrived), w_ckv)
    attn_sum.step(memory_grad)
    attn_sum.step()
    late = after(activated, attn_sum.got_first)
    layer_out = by_seq(low(stream2 + project(late, w_down) + bias_vals[:, 3]))
    mlp_out_grad = after(mlp_out_sum, attn_sum.got_first).astype(jnp.float32)
    attn_sum.own = after(attn_sum.own, layer_out, mlp_out_grad)
    (mlp_in_grad,) = in_sum.results()
    cross_query_grad, cross_kv_grad, cross_out_grad, attn_out_grad = cross_sum.results()
    attn_in_grad, small_grad = attn_sum.results()
    return (
        layer_out,
        input_grad,
        memory_grad,
        attn_in_grad,
        attn_out_grad,
        cross_query_grad,
        cross_kv_grad,
        cross_out_grad,
        mlp_in_grad,
        mlp_out_grad,
        small_grad[:, :3],
        small_grad[:, 3:7],
        small_grad[:, 7:11].reshape(-1),
    )


def solution(mesh):
    in_specs = (
        P(("fsdp", "dp"), None, None),
        P(("fsdp", "dp"), None, None),
        P(("fsdp", "dp")),
        P(("fsdp", "dp"), None, None),
        P(("fsdp", "dp"), None),
        P(("fsdp", "dp"), None),
        P(("fsdp", "dp"), None),
        P(("fsdp", "dp"), None),
        P(("fsdp", "dp"), None),
        P(("fsdp", "dp"), None),
        P(("fsdp", "dp"), None),
        P(("fsdp", "dp"), None),
        P(("fsdp", "dp"), None),
        P(("fsdp", "dp")),
    )
    out_specs = (
        P(("fsdp", "dp"), None, None),
        P(("fsdp", "dp"), None, None),
        P(("fsdp", "dp"), None, None),
        P(("fsdp", "dp"), None),
        P(("fsdp", "dp"), None),
        P(("fsdp", "dp"), None),
        P(("fsdp", "dp"), None),
        P(("fsdp", "dp"), None),
        P(("fsdp", "dp"), None),
        P(("fsdp", "dp"), None),
        P(("fsdp", "dp"), None),
        P(("fsdp", "dp"), None),
        P(("fsdp", "dp")),
    )
    if dict(mesh.shape) == {"fsdp": 8, "dp": 4}:
        program = functools.partial(local, GridGather, GridReduction)
    else:
        program = functools.partial(local, PlainGather, PlainReduction)
    return jax.shard_map(program, mesh=mesh, in_specs=in_specs, out_specs=out_specs, check_vma=False)
```

```python
import functools

import jax
import jax.numpy as jnp
from jax import lax
from jax.experimental import pallas as pl
from jax.experimental.pallas import tpu as pltpu
from jax.sharding import PartitionSpec as P

D = 768
HEADS = 12
HEAD_DIM = 64
PREFIX = 32


EPS = 1e-05


def norm_forward(value_tensor, gain, shift):
    mean = jnp.mean(value_tensor, axis=-1, keepdims=True)
    centred = value_tensor - mean
    spread = jnp.mean(centred * centred, axis=-1, keepdims=True)
    scale_inv = lax.rsqrt(spread + EPS)
    standard = centred * scale_inv
    return (standard * gain + shift, standard, scale_inv)


def norm_backward(upstream_gradient, standard, scale_inv, gain):
    grad_gain = jnp.sum(upstream_gradient * standard, axis=0)
    grad_shift = jnp.sum(upstream_gradient, axis=0)
    inner = upstream_gradient * gain
    first = jnp.mean(inner, axis=-1, keepdims=True)
    second = jnp.mean(inner * standard, axis=-1, keepdims=True)
    return (scale_inv * (inner - first - standard * second), grad_gain, grad_shift)


def project(value_tensor, weight_matrix):
    return jnp.einsum("...h,ht->...t", value_tensor, weight_matrix, preferred_element_type=jnp.float32)


def back_project(upstream_gradient, weight_matrix):
    return jnp.einsum(
        "...j,aj->...a", upstream_gradient, weight_matrix, preferred_element_type=jnp.float32
    )


PAIRS = HEADS // 2
LANES = 2 * HEAD_DIM


def dot(a, b, over):
    return lax.dot_general(a, b, (over, ((), ())), preferred_element_type=jnp.float32)


NATURAL = ((1,), (0,))
BOTH_LAST = ((1,), (1,))
BOTH_FIRST = ((0,), (0,))


def low_lanes(rows):
    return lax.broadcasted_iota(jnp.int32, (rows, LANES), 1) < HEAD_DIM


def stacked(pair, level):
    low = low_lanes(pair.shape[0])
    first = jnp.where(low, level, 0.0).astype(jnp.bfloat16)
    second = jnp.where(low, 0.0, level).astype(jnp.bfloat16)
    return jnp.concatenate([pair * first, pair * second], axis=0)


def unstacked(value):
    rows = value.shape[0] // 2
    return jnp.where(low_lanes(rows), value[:rows], value[rows:])


def lanes_of(ref, start):
    return ref[0, :, start : start + LANES]


def forward_pair(query, key, value, allowed):
    scores = dot(key, stacked(query, HEAD_DIM**-0.5), BOTH_LAST)
    if allowed is not None:
        scores = jnp.where(allowed, scores, -1e30)
    weights = jnp.exp(scores - jnp.max(scores, axis=0, keepdims=True))
    probs = (weights * (1.0 / jnp.sum(weights, axis=0, keepdims=True))).astype(jnp.bfloat16)
    context = unstacked(dot(probs, value, BOTH_FIRST)).astype(jnp.bfloat16)
    return context, probs


def backward_pair(query, key, value, probs, grad):
    scale = HEAD_DIM**-0.5
    grads = stacked(grad, 1.0)
    grad_probs = dot(value, grads, BOTH_LAST)
    wide = probs.astype(jnp.float32)
    delta = jnp.sum(grad_probs * wide, axis=0, keepdims=True)
    grad_scores = (wide * (grad_probs - delta)).astype(jnp.bfloat16)
    grad_key = dot(grad_scores, stacked(query, scale), NATURAL).astype(jnp.bfloat16)
    grad_value = dot(probs, grads, NATURAL).astype(jnp.bfloat16)
    grad_query = (unstacked(dot(grad_scores, key, BOTH_FIRST)) * scale).astype(jnp.bfloat16)
    return grad_query, grad_key, grad_value


def self_forward_body(lens, qkv, context, probs):
    rows = qkv.shape[1]
    at_key = lax.broadcasted_iota(jnp.int32, (rows, 2 * rows), 0)
    at_query = lax.broadcasted_iota(jnp.int32, (rows, 2 * rows), 1)
    at_query = jnp.where(at_query < rows, at_query, at_query - rows)
    allowed = (at_key <= at_query) & (at_key < PREFIX + lens[pl.program_id(0)])
    for p in range(PAIRS):
        at = p * LANES
        out, kept = forward_pair(
            lanes_of(qkv, at), lanes_of(qkv, D + at), lanes_of(qkv, 2 * D + at), allowed
        )
        context[0, :, at : at + LANES] = out
        probs[0, p] = kept


def self_backward_body(qkv, probs, grad, grad_qkv):
    for p in range(PAIRS):
        at = p * LANES
        gq, gk, gv = backward_pair(
            lanes_of(qkv, at),
            lanes_of(qkv, D + at),
            lanes_of(qkv, 2 * D + at),
            probs[0, p],
            lanes_of(grad, at),
        )
        grad_qkv[0, :, at : at + LANES] = gq
        grad_qkv[0, :, D + at : D + at + LANES] = gk
        grad_qkv[0, :, 2 * D + at : 2 * D + at + LANES] = gv


def cross_forward_body(query, kv, context, probs):
    for p in range(PAIRS):
        at = p * LANES
        out, kept = forward_pair(lanes_of(query, at), lanes_of(kv, at), lanes_of(kv, D + at), None)
        context[0, :, at : at + LANES] = out
        probs[0, p] = kept


def cross_backward_body(query, kv, probs, grad, grad_query, grad_kv):
    for p in range(PAIRS):
        at = p * LANES
        gq, gk, gv = backward_pair(
            lanes_of(query, at),
            lanes_of(kv, at),
            lanes_of(kv, D + at),
            probs[0, p],
            lanes_of(grad, at),
        )
        grad_query[0, :, at : at + LANES] = gq
        grad_kv[0, :, at : at + LANES] = gk
        grad_kv[0, :, D + at : D + at + LANES] = gv


def whole_block(shape):
    rest = len(shape) - 1
    return pl.BlockSpec((1,) + tuple(shape[1:]), lambda s, *_: (s,) + (0,) * rest)


def per_sequence(body, name, inputs, shapes, lens=None):
    outs = [jax.ShapeDtypeStruct(shape, jnp.bfloat16) for shape in shapes]
    return pl.pallas_call(
        body,
        out_shape=outs,
        grid_spec=pltpu.PrefetchScalarGridSpec(
            num_scalar_prefetch=0 if lens is None else 1,
            grid=(inputs[0].shape[0],),
            in_specs=[whole_block(v.shape) for v in inputs],
            out_specs=[whole_block(shape) for shape in shapes],
        ),
        name=name,
    )(*(() if lens is None else (lens,)), *inputs)


def self_forward(qkv, lens):
    seqs, rows, _ = qkv.shape
    return per_sequence(
        self_forward_body,
        "self_forward",
        [qkv],
        [(seqs, rows, D), (seqs, PAIRS, rows, 2 * rows)],
        lens,
    )


def self_backward(qkv, probs, grad):
    return per_sequence(self_backward_body, "self_backward", [qkv, probs, grad], [qkv.shape])[0]


def cross_forward(query, kv):
    seqs, rows, _ = query.shape
    return per_sequence(
        cross_forward_body,
        "cross_forward",
        [query, kv],
        [query.shape, (seqs, PAIRS, kv.shape[1], 2 * rows)],
    )


def cross_backward(query, kv, probs, grad):
    return per_sequence(
        cross_backward_body,
        "cross_backward",
        [query, kv, probs, grad],
        [query.shape, kv.shape],
    )


AXES = ("fsdp", "dp")


def grid_rank(z, x, y, core):
    return ((z * 2 + x) * 2 + y) * 2 + core


def grid_perm(move):
    return [
        (grid_rank(z, x, y, core), grid_rank(*move(z, x, y, core)))
        for z in range(4)
        for x in range(2)
        for y in range(2)
        for core in range(2)
    ]


CORE = grid_perm(lambda z, x, y, core: (z, x, y, core ^ 1))
ZNEAR = grid_perm(lambda z, x, y, core: (z ^ 1, x, y, core))
ZFAR = grid_perm(lambda z, x, y, core: (z ^ 2, x, y, core))
FIRST = grid_perm(lambda z, x, y, core: (z, x ^ (1 - core), y ^ core, core))
SECOND = grid_perm(lambda z, x, y, core: (z, x ^ core, y ^ (1 - core), core))


def move(value, perm):
    return lax.ppermute(value, AXES, perm)


def place():
    outer, inner = lax.axis_index("fsdp"), lax.axis_index("dp")
    return outer // 2, outer % 2, inner // 2, inner % 2


def half_of(value, side):
    width = value.shape[-1] // 2
    return lax.dynamic_slice_in_dim(value, side * width, width, axis=-1)


def after(value, *earlier):
    return lax.optimization_barrier((value,) + earlier)[0]


def assemble_body(widths, spot, *refs):
    parts, outs = refs[:8], refs[8:]
    x, y, core = spot[1], spot[2], spot[3]
    for theirs in range(2):
        side = 1 - core if theirs else core
        for j in range(4):
            at_x = x ^ (0, 1 - side, side, 1)[j]
            at_y = y ^ (0, side, 1 - side, 1)[j]
            offset = 0
            for width, out in zip(widths, outs):
                out[0, at_x, at_y, side] = parts[theirs * 4 + j][0, :, offset : offset + width]
                offset += width


def assemble(parts, rows, widths, spot):
    outs = pl.pallas_call(
        functools.partial(assemble_body, widths),
        out_shape=[jax.ShapeDtypeStruct((4, 2, 2, 2, rows, w), jnp.bfloat16) for w in widths],
        grid_spec=pltpu.PrefetchScalarGridSpec(
            num_scalar_prefetch=1,
            grid=(4,),
            in_specs=[pl.BlockSpec((1, rows, sum(widths)), lambda k, spot: (k, 0, 0))] * 8,
            out_specs=[
                pl.BlockSpec(
                    (1, 2, 2, 2, rows, w),
                    lambda k, spot: (spot[0] ^ (2 * lax.rem(k, 2) + k // 2), 0, 0, 0, 0, 0),
                )
                for w in widths
            ],
        ),
        name="assemble",
    )(spot, *parts)
    return [o.reshape(32 * rows, w) for o, w in zip(outs, widths)]


class GridGather:
    def __init__(self, shards):
        self.shards = shards
        self.own = jnp.concatenate(shards, axis=1) if len(shards) > 1 else shards[0]

    def spread(self, *earlier):
        own = after(self.own, *earlier)
        self.two = jnp.stack((self.own, move(own, ZFAR)))
        self.along = (move(self.two, ZNEAR),)
        return self.along

    def cross(self, *earlier):
        self.line = jnp.concatenate((self.two,) + self.along)
        ready = after(self.line, *earlier)
        self.sides = (move(ready, FIRST), move(ready, SECOND))
        return self.sides

    def corner(self, *earlier):
        self.both = (move(after(self.sides[0], *earlier), SECOND),)
        return self.both

    def swap(self):
        parts = (self.line,) + self.sides + self.both
        self.parts = parts + tuple(move(p, CORE) for p in parts)
        return self.parts

    def join(self, *earlier):
        parts = self.parts
        if earlier:
            parts = lax.optimization_barrier(parts + earlier)[: len(parts)]
        rows = self.shards[0].shape[0]
        widths = [s.shape[1] for s in self.shards]
        return assemble(parts, rows, widths, jnp.stack(place()).astype(jnp.int32))


class PlainGather:
    def __init__(self, shards):
        self.shards = shards

    along = ()

    def spread(self, *earlier):
        return ()

    cross = corner = spread

    def swap(self):
        return ()

    def join(self, *earlier):
        widths = [s.shape[1] for s in self.shards]
        whole = lax.all_gather(jnp.concatenate(self.shards, axis=1), AXES, axis=0, tiled=True)
        results = []
        offset = 0
        for width in widths:
            results.append(whole[:, offset : offset + width])
            offset += width
        return results


def split_body(count, which, *refs):
    del which
    keeps, sends, outs = refs[: 2 * count], refs[2 * count : 4 * count], refs[4 * count :]
    for source, out in ((keeps, outs[0]), (sends, outs[1])):
        offset = 0
        for i in range(count):
            width = source[2 * i].shape[-1]
            total = source[2 * i][...].astype(jnp.float32) + source[2 * i + 1][...].astype(
                jnp.float32
            )
            out[:, :, :, offset : offset + width] = total.astype(jnp.bfloat16)
            offset += width


def split_add(pairs, rows):
    z, x, y, core = place()
    first = jnp.where(core == 0, x, y)
    second = jnp.where(core == 0, y, x)
    first_weight = jnp.where(core == 0, 2, 1)
    second_weight = 3 - first_weight
    which = jnp.stack(
        [
            (first ^ f) * first_weight + (second ^ s) * second_weight
            for s in range(2)
            for f in range(2)
        ]
    ).astype(jnp.int32)
    views, keep_specs, send_specs = [], [], []
    for keep, got in pairs:
        width = keep.shape[1]
        block = (4, 1, 2 * rows, width)
        for value in (keep, got):
            views.append(value.reshape(4, 4, 2 * rows, width))
            keep_specs.append(pl.BlockSpec(block, lambda f, which: (0, which[f], 0, 0)))
            send_specs.append(pl.BlockSpec(block, lambda f, which: (0, which[2 + f], 0, 0)))
    total = sum(keep.shape[1] for keep, _ in pairs)
    shape = jax.ShapeDtypeStruct((4, 2, 2 * rows, total), jnp.bfloat16)
    out_spec = pl.BlockSpec((4, 1, 2 * rows, total), lambda f, which: (0, f, 0, 0))
    return pl.pallas_call(
        functools.partial(split_body, len(pairs)),
        out_shape=[shape, shape],
        grid_spec=pltpu.PrefetchScalarGridSpec(
            num_scalar_prefetch=1,
            grid=(2,),
            in_specs=keep_specs + send_specs,
            out_specs=[out_spec, out_spec],
        ),
        name="split_add",
    )(which, *views, *views)


def summed(partial):
    return lax.psum_scatter(partial, AXES, scatter_dimension=0, tiled=True)


class GridReduction:
    def __init__(self, factors):
        core = place()[3]
        self.rows = factors[0][0].shape[-1] // 32
        self.sends = [contract_low(v, half_of(u, 1 - core)) for v, u in factors]
        self.factors = factors
        self.stage = 0

    def add(self, value, upstream_gradient):
        side = 1 - place()[3]
        self.sends.append(contract_low(value, half_of(upstream_gradient, side)))
        self.factors.append((value, upstream_gradient))

    def step(self, *earlier):
        self.stage += 1
        return getattr(self, "hop%d" % self.stage)(*earlier)

    def hop1(self):
        core = place()[3]
        self.got = [move(send, CORE) for send in self.sends]
        self.keeps = [contract_low(v, half_of(u, core)) for v, u in self.factors]
        return self.got

    def hop2(self, *earlier):
        keeps = [after(self.keeps[0], *earlier)] + self.keeps[1:]
        self.keep, send = split_add(list(zip(keeps, self.got)), self.rows)
        self.got = move(send, SECOND)
        return [self.got]

    def hop3(self, *earlier):
        f32 = jnp.float32
        self.got = after(self.got, *earlier)
        total = self.keep[:, 1].astype(f32) + self.got[:, 1].astype(f32)
        self.half = total.astype(jnp.bfloat16)
        self.got_first = move(self.half, FIRST)
        return [self.got_first]

    def hop4(self, *earlier):
        z = place()[0]
        self.got_first = after(self.got_first, *earlier)
        f32 = jnp.float32

        def plane(k):
            at = z ^ k
            pick = lambda v: lax.dynamic_index_in_dim(v, at, 0, keepdims=False).astype(f32)
            return pick(self.keep[:, 0]) + pick(self.got[:, 0]) + pick(self.got_first)

        self.own, self.far = plane(0), plane(2)
        self.near = move(jnp.stack([plane(1), plane(3)]).astype(jnp.bfloat16), ZNEAR)
        return [self.near]

    def hop5(self, *earlier):
        near = after(self.near, *earlier).astype(jnp.float32)
        self.own = self.own + near[0]
        self.turn = (self.far + near[1]).astype(jnp.bfloat16)
        self.last = move(self.turn, ZFAR)
        return [self.last]

    def results(self):
        while self.stage < 5:
            self.step()
        core, rows = place()[3], self.rows
        total = self.own + self.last.astype(jnp.float32)
        mine = lax.dynamic_slice_in_dim(total, core * rows, rows, axis=0)
        other = move(lax.dynamic_slice_in_dim(total, (1 - core) * rows, rows, axis=0), CORE)
        left = jnp.where(core == 0, mine, other)
        right = jnp.where(core == 0, other, mine)
        results = []
        offset = 0
        for keep in self.keeps:
            width = keep.shape[1]
            results.append(
                jnp.concatenate(
                    [left[:, offset : offset + width], right[:, offset : offset + width]], axis=1
                )
            )
            offset += width
        return results


class PlainReduction:
    def __init__(self, factors):
        self.factors = factors
        self.sends = []
        self.keep = self.half = self.got_first = self.turn = self.own = self.last = jnp.zeros((), jnp.bfloat16)

    def add(self, value, upstream_gradient):
        self.factors.append((value, upstream_gradient))

    def step(self, *earlier):
        return []

    def results(self):
        packed = jnp.concatenate([contract_low(v, u) for v, u in self.factors], axis=1)
        total = summed(packed).astype(jnp.float32)
        results = []
        offset = 0
        for _, u in self.factors:
            results.append(total[:, offset : offset + u.shape[-1]])
            offset += u.shape[-1]
        return results


def contract_low(value, upstream_gradient):
    over = tuple(range(value.ndim - 1))
    return lax.dot_general(
        value,
        upstream_gradient,
        ((over, over), ((), ())),
        preferred_element_type=jnp.float32,
    ).astype(jnp.bfloat16)


def local(
    gathering,
    reduction,
    tokens,
    memory,
    suffix_len,
    cotangent,
    attn_in,
    attn_out,
    cross_query,
    cross_kv,
    cross_out,
    mlp_in,
    mlp_out,
    ln_gain,
    shifts,
    mlp_bias,
):
    owned = attn_in.shape[0]
    small = jnp.concatenate(
        [
            ln_gain,
            shifts,
            mlp_bias.reshape(owned, 4),
            jnp.zeros((owned, 256 - 11), jnp.bfloat16),
        ],
        axis=1,
    )
    first = gathering([attn_in, small])
    third = gathering([mlp_in])
    whole = lambda v: lax.all_gather(v, AXES, axis=0, tiled=True)
    w_second = whole(jnp.concatenate([attn_out, cross_query, cross_kv, cross_out], axis=1))
    fourth = gathering([mlp_out])
    third.spread(*first.spread())
    first.cross()
    third.cross(*first.corner())
    first.swap()
    w_qkv, smalls = first.join()
    columns = dot(jnp.eye(16, smalls.shape[1], dtype=jnp.bfloat16), smalls, BOTH_LAST)
    gains, biases, hidden_bias = columns[:3], columns[3:7], columns[7:11].T.reshape(-1)
    seqs, rows, width = tokens.shape
    low = lambda v: v.astype(jnp.bfloat16)
    flat = lambda v: v.reshape(seqs * rows, v.shape[-1])
    by_seq = lambda v: v.reshape(seqs, rows, v.shape[-1])
    live = jnp.arange(rows)[None, :] < (PREFIX + suffix_len)[:, None]
    stream0 = flat(tokens).astype(jnp.float32)
    normed1, standard1, inverse1 = norm_forward(stream0, gains[0], biases[0])
    normed1 = low(normed1)
    fourth.spread(w_qkv)
    qkv = by_seq(low(project(normed1, w_qkv)))
    context, probs = self_forward(qkv, suffix_len)
    third.corner(context)
    third.swap()
    w_out, w_cquery = w_second[:, :D], w_second[:, D : 2 * D]
    w_ckv, w_cout = w_second[:, 2 * D : 4 * D], w_second[:, 4 * D :]
    context = flat(context)
    stream1 = stream0 + project(context, w_out)
    normed2, standard2, inverse2 = norm_forward(stream1, gains[1], biases[1])
    normed2 = low(normed2)
    cquery = by_seq(low(project(normed2, w_cquery)))
    ckv = low(project(memory, w_ckv))
    fourth.cross(cquery)
    ccontext, cprobs = cross_forward(cquery, ckv)
    ccontext = flat(ccontext)
    stream2 = stream1 + project(ccontext, w_cout)
    normed3, standard3, inverse3 = norm_forward(stream2, gains[2], biases[2])
    normed3 = low(normed3)
    (w_in,) = third.join(ccontext)
    fourth.corner(ccontext)
    fourth.swap()
    pre = project(normed3, w_in) + hidden_bias
    activated, gelu_back = jax.vjp(lambda v: jax.nn.gelu(v, approximate=True), pre)
    activated = low(activated)

    upstream = flat(cotangent.astype(jnp.float32) * live[..., None].astype(jnp.float32))
    dout3 = low(upstream)
    down_partial = contract_low(activated, dout3)
    mlp_out_sum = summed(down_partial)
    g_out_bias = jnp.sum(dout3, axis=0, dtype=jnp.float32)
    (w_down,) = fourth.join(down_partial)
    grad_act = back_project(dout3, w_down)
    dpre = low(gelu_back(grad_act)[0])
    g_hidden_bias = jnp.sum(dpre, axis=0, dtype=jnp.float32)
    in_sum = reduction([(normed3, dpre)])
    dpre = after(dpre, *in_sum.sends)
    grad_back, g_gain3, g_shift3 = norm_backward(
        back_project(dpre, w_in), standard3, inverse3, gains[2]
    )
    upstream = upstream + grad_back
    dout2 = low(upstream)
    dccontext = by_seq(low(back_project(dout2, w_cout)))
    in_sum.step()
    arriving = in_sum.step()
    dccontext = after(dccontext, in_sum.keep)
    dcquery, dckv = cross_backward(cquery, ckv, cprobs, dccontext)
    dcq = flat(dcquery)
    cross_sum = reduction([(normed2, dcq), (memory, dckv), (ccontext, dout2)])
    dcq = after(dcq, *arriving, *cross_sum.sends)
    grad_back, g_gain2, g_shift2 = norm_backward(
        back_project(dcq, w_cquery), standard2, inverse2, gains[1]
    )
    upstream = upstream + grad_back
    dout1 = low(upstream)
    attn_sum = reduction([(context, dout1)])
    dcontext = by_seq(low(back_project(dout1, w_out)))
    cross_sum.step()
    crossing = cross_sum.step()
    dcontext = after(dcontext, cross_sum.keep, *attn_sum.sends)
    dqkv = flat(self_backward(qkv, probs, dcontext))
    in_sum.step(dqkv)
    attn_sum.add(normed1, dqkv)
    grad_back, g_gain1, g_shift1 = norm_backward(
        back_project(after(dqkv, *attn_sum.sends, *crossing), w_qkv),
        standard1,
        inverse1,
        gains[0],
    )
    input_grad = by_seq(upstream + grad_back)
    small_sums = jnp.stack(
        (g_gain1, g_gain2, g_gain3, g_shift1, g_shift2, g_shift3, g_out_bias), axis=0
    )
    bias_sums = g_hidden_bias.reshape(D, 4).T
    sums = jnp.concatenate([small_sums, bias_sums], axis=0)
    picks = jnp.eye(11, 256, dtype=jnp.bfloat16)
    attn_sum.add(low(sums), picks)
    attn_sum.step()
    cross_sum.step()
    attn_sum.step()
    attn_sum.step()
    in_sum.step()
    in_sum.step(attn_sum.keep)
    cross_sum.step(attn_sum.keep)
    cross_sum.step(attn_sum.half)
    mlp_out_grad = after(mlp_out_sum, attn_sum.half).astype(jnp.float32)
    attn_sum.step(mlp_out_grad)
    cross_sum.last = after(cross_sum.last, attn_sum.got_first)
    memory_grad = back_project(after(dckv, attn_sum.got_first), w_ckv)
    attn_sum.step(memory_grad)
    late = after(activated, attn_sum.turn)
    layer_out = by_seq(low(stream2 + project(late, w_down) + biases[3]))
    attn_sum.own = after(attn_sum.own, layer_out)
    (mlp_in_grad,) = in_sum.results()
    cross_query_grad, cross_kv_grad, cross_out_grad = cross_sum.results()
    attn_out_grad, attn_in_grad, small_grad = attn_sum.results()
    return (
        layer_out,
        input_grad,
        memory_grad,
        attn_in_grad,
        attn_out_grad,
        cross_query_grad,
        cross_kv_grad,
        cross_out_grad,
        mlp_in_grad,
        mlp_out_grad,
        small_grad[:, :3],
        small_grad[:, 3:7],
        small_grad[:, 7:11].reshape(-1),
    )


def solution(mesh):
    in_specs = (
        P(("fsdp", "dp"), None, None),
        P(("fsdp", "dp"), None, None),
        P(("fsdp", "dp")),
        P(("fsdp", "dp"), None, None),
        P(("fsdp", "dp"), None),
        P(("fsdp", "dp"), None),
        P(("fsdp", "dp"), None),
        P(("fsdp", "dp"), None),
        P(("fsdp", "dp"), None),
        P(("fsdp", "dp"), None),
        P(("fsdp", "dp"), None),
        P(("fsdp", "dp"), None),
        P(("fsdp", "dp"), None),
        P(("fsdp", "dp")),
    )
    out_specs = (
        P(("fsdp", "dp"), None, None),
        P(("fsdp", "dp"), None, None),
        P(("fsdp", "dp"), None, None),
        P(("fsdp", "dp"), None),
        P(("fsdp", "dp"), None),
        P(("fsdp", "dp"), None),
        P(("fsdp", "dp"), None),
        P(("fsdp", "dp"), None),
        P(("fsdp", "dp"), None),
        P(("fsdp", "dp"), None),
        P(("fsdp", "dp"), None),
        P(("fsdp", "dp"), None),
        P(("fsdp", "dp")),
    )
    if dict(mesh.shape) == {"fsdp": 8, "dp": 4}:
        program = functools.partial(local, GridGather, GridReduction)
    else:
        program = functools.partial(local, PlainGather, PlainReduction)
    return jax.shard_map(program, mesh=mesh, in_specs=in_specs, out_specs=out_specs, check_vma=False)
```

```python
import functools

import jax
import jax.numpy as jnp
from jax import lax
from jax.experimental import pallas as pl
from jax.experimental.pallas import tpu as pltpu
from jax.sharding import PartitionSpec as P

D = 768
HEADS = 12
HEAD_DIM = 64
PREFIX = 32


EPS = 1e-05


def norm_forward(value_tensor, gain, shift):
    mean = jnp.mean(value_tensor, axis=-1, keepdims=True)
    centred = value_tensor - mean
    spread = jnp.mean(centred * centred, axis=-1, keepdims=True)
    scale_inv = lax.rsqrt(spread + EPS)
    standard = centred * scale_inv
    return (standard * gain + shift, standard, scale_inv)


def norm_backward(upstream_gradient, standard, scale_inv, gain):
    grad_gain = jnp.sum(upstream_gradient * standard, axis=0)
    grad_shift = jnp.sum(upstream_gradient, axis=0)
    inner = upstream_gradient * gain
    first = jnp.mean(inner, axis=-1, keepdims=True)
    second = jnp.mean(inner * standard, axis=-1, keepdims=True)
    return (scale_inv * (inner - first - standard * second), grad_gain, grad_shift)


def project(value_tensor, weight_matrix):
    return jnp.einsum("...h,ht->...t", value_tensor, weight_matrix, preferred_element_type=jnp.float32)


def back_project(upstream_gradient, weight_matrix):
    return jnp.einsum(
        "...j,aj->...a", upstream_gradient, weight_matrix, preferred_element_type=jnp.float32
    )


PAIRS = HEADS // 2
LANES = 2 * HEAD_DIM


def dot(a, b, over):
    return lax.dot_general(a, b, (over, ((), ())), preferred_element_type=jnp.float32)


NATURAL = ((1,), (0,))
BOTH_LAST = ((1,), (1,))
BOTH_FIRST = ((0,), (0,))


def low_lanes(rows):
    return lax.broadcasted_iota(jnp.int32, (rows, LANES), 1) < HEAD_DIM


def stacked(pair, level):
    low = low_lanes(pair.shape[0])
    first = jnp.where(low, level, 0.0).astype(jnp.bfloat16)
    second = jnp.where(low, 0.0, level).astype(jnp.bfloat16)
    return jnp.concatenate([pair * first, pair * second], axis=0)


def unstacked(value):
    rows = value.shape[0] // 2
    return jnp.where(low_lanes(rows), value[:rows], value[rows:])


def lanes_of(ref, start):
    return ref[0, :, start : start + LANES]


def forward_pair(query, key, value, allowed):
    scores = dot(key, stacked(query, HEAD_DIM**-0.5), BOTH_LAST)
    if allowed is not None:
        scores = jnp.where(allowed, scores, -1e30)
    weights = jnp.exp(scores - jnp.max(scores, axis=0, keepdims=True))
    probs = (weights * (1.0 / jnp.sum(weights, axis=0, keepdims=True))).astype(jnp.bfloat16)
    context = unstacked(dot(probs, value, BOTH_FIRST)).astype(jnp.bfloat16)
    return context, probs


def backward_pair(query, key, value, probs, grad):
    scale = HEAD_DIM**-0.5
    grads = stacked(grad, 1.0)
    grad_probs = dot(value, grads, BOTH_LAST)
    wide = probs.astype(jnp.float32)
    delta = jnp.sum(grad_probs * wide, axis=0, keepdims=True)
    grad_scores = (wide * (grad_probs - delta)).astype(jnp.bfloat16)
    grad_key = dot(grad_scores, stacked(query, scale), NATURAL).astype(jnp.bfloat16)
    grad_value = dot(probs, grads, NATURAL).astype(jnp.bfloat16)
    grad_query = (unstacked(dot(grad_scores, key, BOTH_FIRST)) * scale).astype(jnp.bfloat16)
    return grad_query, grad_key, grad_value


def self_forward_body(lens, qkv, context, probs):
    rows = qkv.shape[1]
    at_key = lax.broadcasted_iota(jnp.int32, (rows, 2 * rows), 0)
    at_query = lax.broadcasted_iota(jnp.int32, (rows, 2 * rows), 1)
    at_query = jnp.where(at_query < rows, at_query, at_query - rows)
    allowed = (at_key <= at_query) & (at_key < PREFIX + lens[pl.program_id(0)])
    for p in range(PAIRS):
        at = p * LANES
        out, kept = forward_pair(
            lanes_of(qkv, at), lanes_of(qkv, D + at), lanes_of(qkv, 2 * D + at), allowed
        )
        context[0, :, at : at + LANES] = out
        probs[0, p] = kept


def self_backward_body(qkv, probs, grad, grad_qkv):
    for p in range(PAIRS):
        at = p * LANES
        gq, gk, gv = backward_pair(
            lanes_of(qkv, at),
            lanes_of(qkv, D + at),
            lanes_of(qkv, 2 * D + at),
            probs[0, p],
            lanes_of(grad, at),
        )
        grad_qkv[0, :, at : at + LANES] = gq
        grad_qkv[0, :, D + at : D + at + LANES] = gk
        grad_qkv[0, :, 2 * D + at : 2 * D + at + LANES] = gv


def cross_forward_body(query, kv, context, probs):
    for p in range(PAIRS):
        at = p * LANES
        out, kept = forward_pair(lanes_of(query, at), lanes_of(kv, at), lanes_of(kv, D + at), None)
        context[0, :, at : at + LANES] = out
        probs[0, p] = kept


def cross_backward_body(query, kv, probs, grad, grad_query, grad_kv):
    for p in range(PAIRS):
        at = p * LANES
        gq, gk, gv = backward_pair(
            lanes_of(query, at),
            lanes_of(kv, at),
            lanes_of(kv, D + at),
            probs[0, p],
            lanes_of(grad, at),
        )
        grad_query[0, :, at : at + LANES] = gq
        grad_kv[0, :, at : at + LANES] = gk
        grad_kv[0, :, D + at : D + at + LANES] = gv


def whole_block(shape):
    rest = len(shape) - 1
    return pl.BlockSpec((1,) + tuple(shape[1:]), lambda s, *_: (s,) + (0,) * rest)


def per_sequence(body, name, inputs, shapes, lens=None):
    outs = [jax.ShapeDtypeStruct(shape, jnp.bfloat16) for shape in shapes]
    return pl.pallas_call(
        body,
        out_shape=outs,
        grid_spec=pltpu.PrefetchScalarGridSpec(
            num_scalar_prefetch=0 if lens is None else 1,
            grid=(inputs[0].shape[0],),
            in_specs=[whole_block(v.shape) for v in inputs],
            out_specs=[whole_block(shape) for shape in shapes],
        ),
        name=name,
    )(*(() if lens is None else (lens,)), *inputs)


def self_forward(qkv, lens):
    seqs, rows, _ = qkv.shape
    return per_sequence(
        self_forward_body,
        "self_forward",
        [qkv],
        [(seqs, rows, D), (seqs, PAIRS, rows, 2 * rows)],
        lens,
    )


def self_backward(qkv, probs, grad):
    return per_sequence(self_backward_body, "self_backward", [qkv, probs, grad], [qkv.shape])[0]


def cross_forward(query, kv):
    seqs, rows, _ = query.shape
    return per_sequence(
        cross_forward_body,
        "cross_forward",
        [query, kv],
        [query.shape, (seqs, PAIRS, kv.shape[1], 2 * rows)],
    )


def cross_backward(query, kv, probs, grad):
    return per_sequence(
        cross_backward_body,
        "cross_backward",
        [query, kv, probs, grad],
        [query.shape, kv.shape],
    )


AXES = ("fsdp", "dp")


def grid_rank(z, x, y, core):
    return ((z * 2 + x) * 2 + y) * 2 + core


def grid_perm(move):
    return [
        (grid_rank(z, x, y, core), grid_rank(*move(z, x, y, core)))
        for z in range(4)
        for x in range(2)
        for y in range(2)
        for core in range(2)
    ]


CORE = grid_perm(lambda z, x, y, core: (z, x, y, core ^ 1))
ZNEAR = grid_perm(lambda z, x, y, core: (z ^ 1, x, y, core))
ZFAR = grid_perm(lambda z, x, y, core: (z ^ 2, x, y, core))
FIRST = grid_perm(lambda z, x, y, core: (z, x ^ (1 - core), y ^ core, core))
SECOND = grid_perm(lambda z, x, y, core: (z, x ^ core, y ^ (1 - core), core))


def move(value, perm):
    return lax.ppermute(value, AXES, perm)


def place():
    outer, inner = lax.axis_index("fsdp"), lax.axis_index("dp")
    return outer // 2, outer % 2, inner // 2, inner % 2


def half_of(value, side):
    width = value.shape[-1] // 2
    return lax.dynamic_slice_in_dim(value, side * width, width, axis=-1)


def after(value, *earlier):
    return lax.optimization_barrier((value,) + earlier)[0]


def assemble_body(widths, spot, *refs):
    parts, outs = refs[:8], refs[8:]
    x, y, core = spot[1], spot[2], spot[3]
    for theirs in range(2):
        side = 1 - core if theirs else core
        for j in range(4):
            at_x = x ^ (0, 1 - side, side, 1)[j]
            at_y = y ^ (0, side, 1 - side, 1)[j]
            offset = 0
            for width, out in zip(widths, outs):
                out[0, at_x, at_y, side] = parts[theirs * 4 + j][0, :, offset : offset + width]
                offset += width


def assemble(parts, rows, widths, spot):
    outs = pl.pallas_call(
        functools.partial(assemble_body, widths),
        out_shape=[jax.ShapeDtypeStruct((4, 2, 2, 2, rows, w), jnp.bfloat16) for w in widths],
        grid_spec=pltpu.PrefetchScalarGridSpec(
            num_scalar_prefetch=1,
            grid=(4,),
            in_specs=[pl.BlockSpec((1, rows, sum(widths)), lambda k, spot: (k, 0, 0))] * 8,
            out_specs=[
                pl.BlockSpec(
                    (1, 2, 2, 2, rows, w),
                    lambda k, spot: (spot[0] ^ (2 * lax.rem(k, 2) + k // 2), 0, 0, 0, 0, 0),
                )
                for w in widths
            ],
        ),
        name="assemble",
    )(spot, *parts)
    return [o.reshape(32 * rows, w) for o, w in zip(outs, widths)]


class GridGather:
    def __init__(self, shards):
        self.shards = shards
        self.own = jnp.concatenate(shards, axis=1) if len(shards) > 1 else shards[0]

    def spread(self, *earlier):
        own = after(self.own, *earlier)
        self.two = jnp.stack((self.own, move(own, ZFAR)))
        self.along = (move(self.two, ZNEAR),)
        return self.along

    def cross(self, *earlier):
        self.line = jnp.concatenate((self.two,) + self.along)
        ready = after(self.line, *earlier)
        self.sides = (move(ready, FIRST), move(ready, SECOND))
        return self.sides

    def corner(self, *earlier):
        self.both = (move(after(self.sides[0], *earlier), SECOND),)
        return self.both

    def swap(self):
        parts = (self.line,) + self.sides + self.both
        self.parts = parts + tuple(move(p, CORE) for p in parts)
        return self.parts

    def join(self, *earlier):
        parts = self.parts
        if earlier:
            parts = lax.optimization_barrier(parts + earlier)[: len(parts)]
        rows = self.shards[0].shape[0]
        widths = [s.shape[1] for s in self.shards]
        return assemble(parts, rows, widths, jnp.stack(place()).astype(jnp.int32))


class PlainGather:
    def __init__(self, shards):
        self.shards = shards

    along = ()

    def spread(self, *earlier):
        return ()

    cross = corner = spread

    def swap(self):
        return ()

    def join(self, *earlier):
        widths = [s.shape[1] for s in self.shards]
        whole = lax.all_gather(jnp.concatenate(self.shards, axis=1), AXES, axis=0, tiled=True)
        results = []
        offset = 0
        for width in widths:
            results.append(whole[:, offset : offset + width])
            offset += width
        return results


def split_body(count, which, *refs):
    del which
    keeps, sends, outs = refs[: 2 * count], refs[2 * count : 4 * count], refs[4 * count :]
    for source, out in ((keeps, outs[0]), (sends, outs[1])):
        offset = 0
        for i in range(count):
            width = source[2 * i].shape[-1]
            total = source[2 * i][...].astype(jnp.float32) + source[2 * i + 1][...].astype(
                jnp.float32
            )
            out[0, :, :, offset : offset + width] = total[:, 0].astype(jnp.bfloat16)
            offset += width


def split_add(pairs, rows):
    z, x, y, core = place()
    first = jnp.where(core == 0, x, y)
    second = jnp.where(core == 0, y, x)
    first_weight = jnp.where(core == 0, 2, 1)
    second_weight = 3 - first_weight
    which = jnp.stack(
        [
            (first ^ f) * first_weight + (second ^ s) * second_weight
            for s in range(2)
            for f in range(2)
        ]
    ).astype(jnp.int32)
    views, keep_specs, send_specs = [], [], []
    for keep, got in pairs:
        width = keep.shape[1]
        block = (4, 1, 2 * rows, width)
        for value in (keep, got):
            views.append(value.reshape(4, 4, 2 * rows, width))
            keep_specs.append(pl.BlockSpec(block, lambda f, which: (0, which[f], 0, 0)))
            send_specs.append(pl.BlockSpec(block, lambda f, which: (0, which[2 + f], 0, 0)))
    total = sum(keep.shape[1] for keep, _ in pairs)
    shape = jax.ShapeDtypeStruct((2, 4, 2 * rows, total), jnp.bfloat16)
    out_spec = pl.BlockSpec((1, 4, 2 * rows, total), lambda f, which: (f, 0, 0, 0))
    return pl.pallas_call(
        functools.partial(split_body, len(pairs)),
        out_shape=[shape, shape],
        grid_spec=pltpu.PrefetchScalarGridSpec(
            num_scalar_prefetch=1,
            grid=(2,),
            in_specs=keep_specs + send_specs,
            out_specs=[out_spec, out_spec],
        ),
        name="split_add",
    )(which, *views, *views)


def summed(partial):
    return lax.psum_scatter(partial, AXES, scatter_dimension=0, tiled=True)


class GridReduction:
    def __init__(self, factors):
        core = place()[3]
        self.rows = factors[0][0].shape[-1] // 32
        self.sends = [contract_low(v, half_of(u, 1 - core)) for v, u in factors]
        self.factors = factors
        self.stage = 0

    def add(self, value, upstream_gradient):
        side = 1 - place()[3]
        self.sends.append(contract_low(value, half_of(upstream_gradient, side)))
        self.factors.append((value, upstream_gradient))

    def step(self, *earlier):
        self.stage += 1
        return getattr(self, "hop%d" % self.stage)(*earlier)

    def hop1(self):
        core = place()[3]
        self.got = [move(send, CORE) for send in self.sends]
        self.keeps = [contract_low(v, half_of(u, core)) for v, u in self.factors]
        return self.got

    def hop2(self, *earlier):
        keeps = [after(self.keeps[0], *earlier)] + self.keeps[1:]
        self.keep, send = split_add(list(zip(keeps, self.got)), self.rows)
        self.got = move(send, SECOND)
        return [self.got]

    def hop3(self, *earlier):
        f32 = jnp.float32
        self.got = after(self.got, *earlier)
        total = self.keep[1].astype(f32) + self.got[1].astype(f32)
        self.half = total.astype(jnp.bfloat16)
        self.got_first = move(self.half, FIRST)
        return [self.got_first]

    def hop4(self, *earlier):
        z = place()[0]
        self.got_first = after(self.got_first, *earlier)
        f32 = jnp.float32

        def plane(k):
            at = z ^ k
            pick = lambda v: lax.dynamic_slice(v, (0, at, 0, 0), (1, 1) + v.shape[2:])[0, 0]
            first = lax.dynamic_index_in_dim(self.got_first, at, 0, keepdims=False)
            return pick(self.keep).astype(f32) + pick(self.got).astype(f32) + first.astype(f32)

        self.own, self.far = plane(0), plane(2)
        self.near = move(jnp.stack([plane(1), plane(3)]).astype(jnp.bfloat16), ZNEAR)
        return [self.near]

    def hop5(self, *earlier):
        near = after(self.near, *earlier).astype(jnp.float32)
        self.own = self.own + near[0]
        self.turn = (self.far + near[1]).astype(jnp.bfloat16)
        self.last = move(self.turn, ZFAR)
        return [self.last]

    def results(self):
        while self.stage < 5:
            self.step()
        core, rows = place()[3], self.rows
        total = self.own + self.last.astype(jnp.float32)
        mine = lax.dynamic_slice_in_dim(total, core * rows, rows, axis=0)
        other = move(lax.dynamic_slice_in_dim(total, (1 - core) * rows, rows, axis=0), CORE)
        left = jnp.where(core == 0, mine, other)
        right = jnp.where(core == 0, other, mine)
        results = []
        offset = 0
        for keep in self.keeps:
            width = keep.shape[1]
            results.append(
                jnp.concatenate(
                    [left[:, offset : offset + width], right[:, offset : offset + width]], axis=1
                )
            )
            offset += width
        return results


class PlainReduction:
    def __init__(self, factors):
        self.factors = factors
        self.sends = []
        self.keep = self.half = self.got_first = self.turn = self.own = self.last = jnp.zeros((), jnp.bfloat16)

    def add(self, value, upstream_gradient):
        self.factors.append((value, upstream_gradient))

    def step(self, *earlier):
        return []

    def results(self):
        packed = jnp.concatenate([contract_low(v, u) for v, u in self.factors], axis=1)
        total = summed(packed).astype(jnp.float32)
        results = []
        offset = 0
        for _, u in self.factors:
            results.append(total[:, offset : offset + u.shape[-1]])
            offset += u.shape[-1]
        return results


def contract_low(value, upstream_gradient):
    over = tuple(range(value.ndim - 1))
    return lax.dot_general(
        value,
        upstream_gradient,
        ((over, over), ((), ())),
        preferred_element_type=jnp.float32,
    ).astype(jnp.bfloat16)


def local(
    gathering,
    reduction,
    tokens,
    memory,
    suffix_len,
    cotangent,
    attn_in,
    attn_out,
    cross_query,
    cross_kv,
    cross_out,
    mlp_in,
    mlp_out,
    ln_gain,
    shifts,
    mlp_bias,
):
    owned = attn_in.shape[0]
    small = jnp.concatenate(
        [
            ln_gain,
            shifts,
            mlp_bias.reshape(owned, 4),
            jnp.zeros((owned, 256 - 11), jnp.bfloat16),
        ],
        axis=1,
    )
    first = gathering([attn_in, small])
    third = gathering([mlp_in])
    whole = lambda v: lax.all_gather(v, AXES, axis=0, tiled=True)
    w_second = whole(jnp.concatenate([attn_out, cross_query, cross_kv, cross_out], axis=1))
    fourth = gathering([mlp_out])
    third.spread(*first.spread())
    first.cross()
    third.cross(*first.corner())
    first.swap()
    w_qkv, smalls = first.join()
    columns = dot(jnp.eye(16, smalls.shape[1], dtype=jnp.bfloat16), smalls, BOTH_LAST)
    gains, biases, hidden_bias = columns[:3], columns[3:7], columns[7:11].T.reshape(-1)
    seqs, rows, width = tokens.shape
    low = lambda v: v.astype(jnp.bfloat16)
    flat = lambda v: v.reshape(seqs * rows, v.shape[-1])
    by_seq = lambda v: v.reshape(seqs, rows, v.shape[-1])
    live = jnp.arange(rows)[None, :] < (PREFIX + suffix_len)[:, None]
    stream0 = flat(tokens).astype(jnp.float32)
    normed1, standard1, inverse1 = norm_forward(stream0, gains[0], biases[0])
    normed1 = low(normed1)
    fourth.spread(w_qkv)
    qkv = by_seq(low(project(normed1, w_qkv)))
    context, probs = self_forward(qkv, suffix_len)
    third.corner(context)
    third.swap()
    w_out, w_cquery = w_second[:, :D], w_second[:, D : 2 * D]
    w_ckv, w_cout = w_second[:, 2 * D : 4 * D], w_second[:, 4 * D :]
    context = flat(context)
    stream1 = stream0 + project(context, w_out)
    normed2, standard2, inverse2 = norm_forward(stream1, gains[1], biases[1])
    normed2 = low(normed2)
    cquery = by_seq(low(project(normed2, w_cquery)))
    ckv = low(project(memory, w_ckv))
    fourth.cross(cquery)
    ccontext, cprobs = cross_forward(cquery, ckv)
    ccontext = flat(ccontext)
    stream2 = stream1 + project(ccontext, w_cout)
    normed3, standard3, inverse3 = norm_forward(stream2, gains[2], biases[2])
    normed3 = low(normed3)
    (w_in,) = third.join(ccontext)
    fourth.corner(ccontext)
    fourth.swap()
    pre = project(normed3, w_in) + hidden_bias
    activated, gelu_back = jax.vjp(lambda v: jax.nn.gelu(v, approximate=True), pre)
    activated = low(activated)

    upstream = flat(cotangent.astype(jnp.float32) * live[..., None].astype(jnp.float32))
    dout3 = low(upstream)
    down_partial = contract_low(activated, dout3)
    mlp_out_sum = summed(down_partial)
    g_out_bias = jnp.sum(dout3, axis=0, dtype=jnp.float32)
    (w_down,) = fourth.join(down_partial)
    grad_act = back_project(dout3, w_down)
    dpre = low(gelu_back(grad_act)[0])
    g_hidden_bias = jnp.sum(dpre, axis=0, dtype=jnp.float32)
    in_sum = reduction([(normed3, dpre)])
    dpre = after(dpre, *in_sum.sends)
    grad_back, g_gain3, g_shift3 = norm_backward(
        back_project(dpre, w_in), standard3, inverse3, gains[2]
    )
    upstream = upstream + grad_back
    dout2 = low(upstream)
    dccontext = by_seq(low(back_project(dout2, w_cout)))
    in_sum.step()
    arriving = in_sum.step()
    dccontext = after(dccontext, in_sum.keep)
    dcquery, dckv = cross_backward(cquery, ckv, cprobs, dccontext)
    dcq = flat(dcquery)
    cross_sum = reduction([(normed2, dcq), (memory, dckv), (ccontext, dout2)])
    dcq = after(dcq, *arriving, *cross_sum.sends)
    grad_back, g_gain2, g_shift2 = norm_backward(
        back_project(dcq, w_cquery), standard2, inverse2, gains[1]
    )
    upstream = upstream + grad_back
    dout1 = low(upstream)
    attn_sum = reduction([(context, dout1)])
    dcontext = by_seq(low(back_project(dout1, w_out)))
    cross_sum.step()
    crossing = cross_sum.step()
    dcontext = after(dcontext, cross_sum.keep, *attn_sum.sends)
    dqkv = flat(self_backward(qkv, probs, dcontext))
    in_sum.step(dqkv)
    attn_sum.add(normed1, dqkv)
    grad_back, g_gain1, g_shift1 = norm_backward(
        back_project(after(dqkv, *attn_sum.sends, *crossing), w_qkv),
        standard1,
        inverse1,
        gains[0],
    )
    input_grad = by_seq(upstream + grad_back)
    small_sums = jnp.stack(
        (g_gain1, g_gain2, g_gain3, g_shift1, g_shift2, g_shift3, g_out_bias), axis=0
    )
    bias_sums = g_hidden_bias.reshape(D, 4).T
    sums = jnp.concatenate([small_sums, bias_sums], axis=0)
    picks = jnp.eye(11, 256, dtype=jnp.bfloat16)
    attn_sum.add(low(sums), picks)
    attn_sum.step()
    cross_sum.step()
    attn_sum.step()
    attn_sum.step()
    in_sum.step()
    in_sum.step(attn_sum.keep)
    cross_sum.step(attn_sum.keep)
    cross_sum.step(attn_sum.half)
    mlp_out_grad = after(mlp_out_sum, attn_sum.half).astype(jnp.float32)
    attn_sum.step(mlp_out_grad)
    memory_grad = back_project(after(dckv, attn_sum.got_first), w_ckv)
    attn_sum.step(memory_grad)
    cross_sum.last = after(cross_sum.last, attn_sum.turn)
    in_sum.last = after(in_sum.last, attn_sum.half)
    late = after(activated, attn_sum.turn)
    layer_out = by_seq(low(stream2 + project(late, w_down) + biases[3]))
    attn_sum.own = after(attn_sum.own, layer_out)
    (mlp_in_grad,) = in_sum.results()
    cross_query_grad, cross_kv_grad, cross_out_grad = cross_sum.results()
    attn_out_grad, attn_in_grad, small_grad = attn_sum.results()
    return (
        layer_out,
        input_grad,
        memory_grad,
        attn_in_grad,
        attn_out_grad,
        cross_query_grad,
        cross_kv_grad,
        cross_out_grad,
        mlp_in_grad,
        mlp_out_grad,
        small_grad[:, :3],
        small_grad[:, 3:7],
        small_grad[:, 7:11].reshape(-1),
    )


def solution(mesh):
    in_specs = (
        P(("fsdp", "dp"), None, None),
        P(("fsdp", "dp"), None, None),
        P(("fsdp", "dp")),
        P(("fsdp", "dp"), None, None),
        P(("fsdp", "dp"), None),
        P(("fsdp", "dp"), None),
        P(("fsdp", "dp"), None),
        P(("fsdp", "dp"), None),
        P(("fsdp", "dp"), None),
        P(("fsdp", "dp"), None),
        P(("fsdp", "dp"), None),
        P(("fsdp", "dp"), None),
        P(("fsdp", "dp"), None),
        P(("fsdp", "dp")),
    )
    out_specs = (
        P(("fsdp", "dp"), None, None),
        P(("fsdp", "dp"), None, None),
        P(("fsdp", "dp"), None, None),
        P(("fsdp", "dp"), None),
        P(("fsdp", "dp"), None),
        P(("fsdp", "dp"), None),
        P(("fsdp", "dp"), None),
        P(("fsdp", "dp"), None),
        P(("fsdp", "dp"), None),
        P(("fsdp", "dp"), None),
        P(("fsdp", "dp"), None),
        P(("fsdp", "dp"), None),
        P(("fsdp", "dp")),
    )
    if dict(mesh.shape) == {"fsdp": 8, "dp": 4}:
        program = functools.partial(local, GridGather, GridReduction)
    else:
        program = functools.partial(local, PlainGather, PlainReduction)
    return jax.shard_map(program, mesh=mesh, in_specs=in_specs, out_specs=out_specs, check_vma=False)
```
